256 devices in a mesh: pts: 64 (over z, x, core), poly: 4 (over y).
Axes of the slice: x: 4, y: 4, z: 8, core: 2. Of those that a mesh axis runs over, the one named last changes fastest.
Arguments:
- points: float32 [2, 524288], P(None, 'pts'), may hold values from 0 to 64, as said below
- segments: float32 [4, 8388608], P(None, ('pts', 'poly')), may hold values from -2.1 to 66.1, as said below
- edge_polygon: int32 [8388608], P(('pts', 'poly')), may hold values from 0 to 32767
- polygon_value: float32 [32768], replicated, may hold values from -6 to 6
- block_pairs: int32 [64, 3, 2, 8], P('pts'), may hold values from 0 to 127, as said below
- live_slots: int32 [64, 3], P('pts'), may hold values from 2 to 8, as said below
Outputs:
- min_sq: float32 [524288], P('pts')
- soft_label: float32 [524288], P('pts')
The draws below stay inside these ranges and needn't reach their ends.
Inputs may be any that keep to these rules, and one draw needn't show every extreme that they name: `points`: point i lies in cell c = i // 8192: its x lies from c to c + 1, its y from 0 to 1. `segments`: edge e belongs to cell c = e // 131072: its start x lies from c - 2 to c + 3, its start y from 0 to 1, and its length from 0.02 to 0.1. block_pairs[c, r, 0, k] is a point block below 8; block_pairs[c, r, 1, k] is below 64 for r = 0 and below 128 otherwise, and the cell that it names always lies in the grid. For r >= 1, slot 0 names a block of cell c + r and slot 1 one of cell c - r wherever that cell lies in the grid. `live_slots`: at least two slots are used; in every cycle some cell uses all 8 slots.
All inputs are finite; a program needn't handle non-finite values.
Results may differ from the reference program's by a relative error of at most 0.0003.
Values sent between devices are 32-bit elements; how exact they have to be, the bound alone decides.
No kernel may reach another device: no remote copies, remote signals or barrier semaphores. Data moves between devices by JAX's collectives and lax.ppermute only.
A program may use at most 64 MiB of HBM per device.

```python
import math
import jax
import jax.numpy as jnp
from jax import lax

PB = 8
BP = 1024
BE = 512
EB = 64
SLOTS = 8
CYCLES = 3
POLYGONS = 32768
POINTS = 524288
EDGES = 8388608
N_PTS = 64
N_POLY = 4


def draw_points(key, part):
    keys = jax.random.split(key, 2)
    cell_of = (jnp.arange(POINTS) // (PB * BP)).astype(jnp.float32)
    offset_x = jax.random.uniform(keys[0], (POINTS,), jnp.float32)
    coord_y = jax.random.uniform(keys[1], (POINTS,), jnp.float32)
    return jnp.stack([cell_of + offset_x * 0.999, coord_y])


def draw_segments(key, part):
    keys = jax.random.split(key, 4)
    cell_of = (jnp.arange(EDGES) // (N_POLY * EB * BE)).astype(jnp.float32)
    spread = 2.0 * CYCLES - 1.0
    start_x = cell_of - (CYCLES - 1.0) + spread * jax.random.uniform(keys[0], (EDGES,), jnp.float32)
    start_y = jax.random.uniform(keys[1], (EDGES,), jnp.float32)
    length = jax.random.uniform(keys[2], (EDGES,), jnp.float32, 0.02, 0.1)
    heading = jax.random.uniform(keys[3], (EDGES,), jnp.float32, -math.pi, math.pi)
    return jnp.stack([start_x, start_y, start_x + length * jnp.cos(heading), start_y + length * jnp.sin(heading)])


def draw_block_pairs(key, part):
    keys = jax.random.split(key, 3)
    shape = (N_PTS, CYCLES, SLOTS)
    point_block = jax.random.randint(keys[0], shape, 0, PB)
    side = jax.random.randint(keys[1], shape, 0, 2)
    within = jax.random.randint(keys[2], shape, 0, EB)
    cell_index = jnp.arange(N_PTS, dtype=jnp.int32)[:, None, None]
    cycle_index = jnp.arange(CYCLES, dtype=jnp.int32)[None, :, None]
    slot_index = jnp.arange(SLOTS, dtype=jnp.int32)[None, None, :]
    side = jnp.where(slot_index == 0, 1, jnp.where(slot_index == 1, 0, side))
    lower_ok = cell_index - cycle_index >= 0
    upper_ok = cell_index + cycle_index <= N_PTS - 1
    side = jnp.where(lower_ok & upper_ok, side, jnp.where(lower_ok, 0, 1))
    side = jnp.where(cycle_index == 0, 0, side)
    return jnp.stack([point_block, side * EB + within], axis=2).astype(jnp.int32)


def draw_live_slots(key, part):
    keys = jax.random.split(key, 2)
    counts = jax.random.randint(keys[0], (N_PTS, CYCLES), 2, SLOTS + 1)
    busiest = jax.random.randint(keys[1], (1, CYCLES), 0, N_PTS)
    cell_index = jnp.arange(N_PTS, dtype=jnp.int32)[:, None]
    return jnp.where(cell_index == busiest, SLOTS, counts).astype(jnp.int32)


def set_ends(result, own_key, smallest, largest):
    spot = [jax.random.randint(jax.random.fold_in(own_key, axis), (), 0, length) for axis, length in enumerate(result.shape)]
    widest = result.shape.index(max(result.shape))
    next_to = spot[:widest] + [(spot[widest] + 1) % result.shape[widest]] + spot[widest + 1:]
    return result.at[tuple(spot)].set(smallest).at[tuple(next_to)].set(largest)


def scatter_about(stream_key, shape, deviation, reach, kind=jnp.bfloat16):
    return jnp.clip(deviation * jax.random.normal(stream_key, shape, jnp.float32), -reach, reach).astype(kind)


def setup_inputs(seed: int = 0) -> dict:
    splits = jax.random.split(jax.random.key(seed), 7)
    points = draw_points(jax.random.fold_in(splits[6], 71), 0)
    segments = draw_segments(jax.random.fold_in(splits[6], 71), 0)
    edge_polygon = set_ends(jax.random.randint(splits[2], (EDGES,), 0, POLYGONS), jax.random.fold_in(splits[2], 1), 0, POLYGONS - 1).astype(jnp.int32)
    polygon_value = scatter_about(splits[3], (POLYGONS,), 1.0, 6.0, jnp.float32)
    block_pairs = draw_block_pairs(jax.random.fold_in(splits[6], 71), 0)
    live_slots = draw_live_slots(jax.random.fold_in(splits[6], 71), 0)
    return dict(points=points, segments=segments, edge_polygon=edge_polygon, polygon_value=polygon_value, block_pairs=block_pairs, live_slots=live_slots)


cutoff = 9.0
smoothing_scale = 9.0 / 256.0


def combine(closest_shape, second_closest_shape):
    minimal_separation = jnp.minimum(closest_shape[0], second_closest_shape[0])
    closest_share = jnp.exp((minimal_separation - closest_shape[0]) / smoothing_scale)
    second_closest_share = jnp.exp((minimal_separation - second_closest_shape[0]) / smoothing_scale)
    return (minimal_separation, closest_shape[1] * closest_share + second_closest_shape[1] * second_closest_share, closest_shape[2] * closest_share + second_closest_shape[2] * second_closest_share)


def segment_terms(point_x, point_y, edge_block):
    start_x = edge_block[0]
    start_y = edge_block[1]
    delta_x = edge_block[2] - start_x
    delta_y = edge_block[3] - start_y
    rel_x = point_x - start_x
    rel_y = point_y - start_y
    fraction = jnp.clip((rel_x * delta_x + rel_y * delta_y) / (delta_x * delta_x + delta_y * delta_y), 0.0, 1.0)
    off_x = rel_x - fraction * delta_x
    off_y = rel_y - fraction * delta_y
    separation_power_two = off_x * off_x + off_y * off_y
    minimal_separation = jnp.min(separation_power_two, axis=-1)
    class_share = jnp.exp((minimal_separation[..., None] - separation_power_two) / smoothing_scale)
    return minimal_separation, jnp.sum(class_share, axis=-1), jnp.sum(class_share * edge_block[4], axis=-1)


def reference(points, segments, edge_polygon, polygon_value, block_pairs, live_slots):
    point_grid = points.reshape(2, N_PTS, PB, BP)
    edge_value = polygon_value[edge_polygon]
    every_edge = jnp.concatenate([segments, edge_value[None, :]], axis=0).reshape(5, N_PTS, N_POLY, EB, BE)
    zero_index = jnp.zeros((), jnp.int32)

    def one_cell(cell_index):
        own_points = lax.dynamic_index_in_dim(point_grid, cell_index, 1, keepdims=False)
        cell_pairs = lax.dynamic_index_in_dim(block_pairs, cell_index, 0, keepdims=False)
        cell_live = lax.dynamic_index_in_dim(live_slots, cell_index, 0, keepdims=False)
        running = (jnp.full((PB, BP), cutoff, jnp.float32), jnp.zeros((PB, BP), jnp.float32), jnp.zeros((PB, BP), jnp.float32))
        for cycle_index in range(CYCLES):
            slot_pairs = cell_pairs[cycle_index]

            def add_slot(slot_index, state):
                point_block = slot_pairs[0, slot_index].astype(jnp.int32)
                named = slot_pairs[1, slot_index].astype(jnp.int32)
                if cycle_index == 0:
                    source_cell = cell_index
                    edge_index = named
                else:
                    source_cell = jnp.where(named < EB, cell_index - cycle_index, cell_index + cycle_index)
                    edge_index = jnp.where(named < EB, named, named - EB)
                starts = (zero_index, source_cell.astype(jnp.int32), zero_index, edge_index.astype(jnp.int32), zero_index)
                edge_block = lax.dynamic_slice(every_edge, starts, (5, 1, N_POLY, 1, BE)).reshape(5, N_POLY, 1, BE)
                coords = lax.dynamic_index_in_dim(own_points, point_block, 1, keepdims=False)
                shard_terms = segment_terms(coords[0][None, :, None], coords[1][None, :, None], edge_block)
                merged = (shard_terms[0][0], shard_terms[1][0], shard_terms[2][0])
                for shard_index in range(1, N_POLY):
                    merged = combine(merged, (shard_terms[0][shard_index], shard_terms[1][shard_index], shard_terms[2][shard_index]))
                current = (lax.dynamic_index_in_dim(state[0], point_block, 0, keepdims=False), lax.dynamic_index_in_dim(state[1], point_block, 0, keepdims=False), lax.dynamic_index_in_dim(state[2], point_block, 0, keepdims=False))
                joined = combine(current, merged)
                return (lax.dynamic_update_index_in_dim(state[0], joined[0], point_block, 0), lax.dynamic_update_index_in_dim(state[1], joined[1], point_block, 0), lax.dynamic_update_index_in_dim(state[2], joined[2], point_block, 0))

            running = lax.fori_loop(jnp.zeros((), jnp.int32), cell_live[cycle_index].astype(jnp.int32), add_slot, running)
        background = (jnp.full((PB, BP), cutoff, jnp.float32), jnp.ones((PB, BP), jnp.float32), jnp.zeros((PB, BP), jnp.float32))
        final_state = combine(running, background)
        return final_state[0], final_state[2] / final_state[1]

    minimal_separation, labels = lax.map(one_cell, jnp.arange(N_PTS, dtype=jnp.int32))
    return minimal_separation.reshape(-1), labels.reshape(-1)
```

```python
import math

import jax
import jax.numpy as jnp
from jax import lax
from jax.experimental import pallas as pl
from jax.experimental.pallas import tpu as pltpu
from jax.sharding import PartitionSpec as P

BP = 1024
BE = 512
EB = 64
SLOTS = 8
CUTOFF = 9.0
SCALE = 256.0 / 9.0 / math.log(2.0)
ROOT = math.sqrt(SCALE)
FAR = CUTOFF * SCALE
OFFSET = 110.0
SAFE = 200.0
UNSEEN = 1.0e30

SMEM = pl.BlockSpec(memory_space=pltpu.SMEM)
VMEM = pl.BlockSpec(memory_space=pltpu.VMEM)


def from_behind(shard, axis, by):
    devices = lax.axis_size(axis)
    pairs = [(i, i + by) for i in range(devices) if 0 <= i + by < devices]
    return lax.ppermute(shard, axis, pairs)


def pick_kernel(own_names, above1, below1, above2, below2, seg, poly, *outs):
    lists = ((own_names, 0), (above1, 1), (below1, 1), (above2, 2), (below2, 2))
    for (names, cycle), out in zip(lists, outs):
        for s in range(SLOTS):
            block = names[0, cycle, 1, s] & (EB - 1)
            start = pl.multiple_of(block * BE, BE)
            for c in range(4):
                out[c, pl.ds(s, 1), :] = seg[pl.ds(c, 1), pl.ds(start, BE)]
            for j in range(BE // 128):
                row = poly[pl.ds(block * (BE // 128) + j, 1), :]
                out[4, pl.ds(s, 1), pl.ds(j * 128, 128)] = row.astype(jnp.float32)


def pick(block_pairs, lists, segments, edge_polygon):
    shape = jax.ShapeDtypeStruct((5, SLOTS, BE), jnp.float32)
    return pl.pallas_call(
        pick_kernel,
        out_shape=[shape] * 5,
        in_specs=[SMEM] * 5 + [VMEM] * 2,
        out_specs=[VMEM] * 5,
        cost_estimate=pl.CostEstimate(flops=1 << 20, bytes_accessed=1 << 20, transcendentals=0),
        name="pick",
    )(block_pairs, *lists, segments, edge_polygon.reshape(-1, 128))


def pieces(x):
    first = x.astype(jnp.bfloat16).astype(jnp.float32)
    rest = x - first
    second = rest.astype(jnp.bfloat16).astype(jnp.float32)
    return first, second, rest - second


def affine_rows(x_factor, y_factor, constant):
    x, y, c = pieces(x_factor), pieces(y_factor), pieces(constant)
    zero = jnp.zeros_like(x_factor)
    rows = [x[0], x[0], x[1], x[1], x[0], x[2], y[0], y[0], y[1], y[1], y[0], y[2], c[0], c[1], c[2], zero]
    return jnp.concatenate(rows, axis=0)


def look_up(table, indices):
    high = indices >> 7
    low = indices & 127
    tiles = BE // 128
    lows = [low[:, 128 * j : 128 * (j + 1)] for j in range(tiles)]
    highs = [high[:, 128 * j : 128 * (j + 1)] for j in range(tiles)]
    unroll = 32

    def step(i, found):
        for k in range(unroll):
            r = i * unroll + k
            row = jnp.broadcast_to(table[pl.ds(r, 1), :], (8, 128))
            found = tuple(
                jnp.where(
                    highs[j] == r,
                    jnp.take_along_axis(row, lows[j], axis=1, mode="promise_in_bounds"),
                    found[j],
                )
                for j in range(tiles)
            )
        return found

    start = tuple(jnp.zeros((8, 128), jnp.float32) for _ in range(tiles))
    found = lax.fori_loop(0, table.shape[0] // unroll, step, start)
    return jnp.concatenate(found, axis=1)


def prepare(raw, table, centre_x, left):
    value = look_up(table, raw[4].astype(jnp.int32))
    start_x, start_y = raw[0], raw[1]
    delta_x = raw[2] - start_x
    delta_y = raw[3] - start_y
    middle_x = (start_x - centre_x) + 0.5 * delta_x
    middle_y = (start_y - 0.5) + 0.5 * delta_y
    squared = jnp.maximum(delta_x * delta_x + delta_y * delta_y, 1e-12)
    inverse = lax.rsqrt(squared) * ROOT
    along_x = delta_x * inverse
    along_y = delta_y * inverse
    half = 0.5 * squared * inverse
    parts = (
        affine_rows(along_x, along_y, -(middle_x * along_x + middle_y * along_y)),
        affine_rows(-along_y, along_x, middle_x * along_y - middle_y * along_x),
        jnp.concatenate(
            list(pieces(half) + pieces(value)) + [jnp.zeros_like(half)] * 10, axis=0
        ),
    )
    for i, part in enumerate(parts):
        left[pl.ds(i * BE, BE), :] = part.T.astype(jnp.bfloat16)


def fill_right(points, centre_x, right, right_const):
    ones = jnp.ones((1, BP), jnp.float32)
    for p in range(8):
        px = pieces(points[0:1, p * BP : (p + 1) * BP] - centre_x)
        py = pieces(points[1:2, p * BP : (p + 1) * BP] - 0.5)
        rows = []
        for q in (px, py):
            rows += [q[0], q[1], q[0], q[1], q[2], q[0]]
        rows += [ones, ones, ones, jnp.zeros_like(ones)]
        full = jnp.concatenate([jnp.broadcast_to(r, (8, BP)) for r in rows], axis=0)
        right[p] = full.astype(jnp.bfloat16)
    row = lax.broadcasted_iota(jnp.int32, (128, 256), 0) // 8
    lane = lax.broadcasted_iota(jnp.int32, (128, 256), 1)
    first = jnp.where(lane < 128, 0, 3)
    const = jnp.where((row >= first) & (row < first + 3), 1.0, 0.0)
    right_const[...] = const.astype(jnp.bfloat16)


def squared_distance(u, v, half):
    beyond = u - jnp.minimum(jnp.maximum(u, -half), half)
    return v * v + beyond * beyond


def join_kernel(cycles, pairs, live, points, table, *refs):
    raws, refs = refs[: 2 * len(cycles)], refs[2 * len(cycles) :]
    out, left, right, right_const, masked, spread, even, odd, m_ref, s_ref, t_ref = refs
    centre_x = points[0:1, 0:1]
    fill_right(points, centre_x, right, right_const)
    slot_row = lax.broadcasted_iota(jnp.int32, (8, BE), 0)
    for i, cycle in enumerate(cycles):
        if cycle == 0:
            raw = [raws[0][c] for c in range(5)]
        else:
            lower = jnp.zeros((8, BE), jnp.int32)
            for s in range(SLOTS):
                side = (pairs[0, cycle, 1, s] < EB).astype(jnp.int32)
                lower = jnp.where(slot_row == s, side, lower)
            raw = [jnp.where(lower > 0, raws[2 * i][c], raws[2 * i + 1][c]) for c in range(5)]
        prepare(raw, table, centre_x, left.at[i])
    m_ref[...] = jnp.full_like(m_ref, UNSEEN)
    s_ref[...] = jnp.zeros_like(s_ref)
    t_ref[...] = jnp.zeros_like(t_ref)

    counts = [live[0, cycle] for cycle in cycles]
    total = sum(counts[1:], counts[0])
    lane = lax.broadcasted_iota(jnp.int32, (1, 128), 1) & 7
    bufs = (even, odd)

    def locate(q):
        if len(cycles) == 1:
            return 0, cycles[0], q
        later = (q >= counts[0]).astype(jnp.int32)
        return later, cycles[0] + later, q - later * counts[0]

    def load(q):
        i, cycle, k = locate(q)
        mask = (lane == k).astype(jnp.bfloat16)
        masked[...] = left[i] * mask
        spread[...] = jnp.dot(
            masked[2 * BE :, :], right_const[...], preferred_element_type=jnp.float32
        )

    def block_of(q):
        _, cycle, k = locate(q)
        return pairs[0, cycle, 0, k]

    def multiply(p, n, buf):
        buf[...] = jnp.dot(
            masked[: 2 * BE, :],
            right[p, :, 256 * n : 256 * (n + 1)],
            preferred_element_type=jnp.float32,
        )

    def slot(q, carry):
        p = block_of(q)
        load(q)
        multiply(p, 0, even)
        for n in range(4):
            if n < 3:
                multiply(p, n + 1, bufs[(n + 1) % 2])
            buf = bufs[n % 2]
            m = s = t = None
            for g in range(BE // 8):
                half = spread[8 * g : 8 * g + 8, 0:128]
                value = spread[8 * g : 8 * g + 8, 128:256]
                half = jnp.concatenate([half, half], axis=1)
                value = jnp.concatenate([value, value], axis=1)
                d = squared_distance(
                    buf[8 * g : 8 * g + 8, :], buf[BE + 8 * g : BE + 8 * g + 8, :], half
                )
                w = jnp.exp2(OFFSET - d)
                m = d if m is None else jnp.minimum(m, d)
                s = w if s is None else s + w
                t = w * value if t is None else t + w * value
            m = jnp.min(m, axis=0, keepdims=True)
            s = jnp.sum(s, axis=0, keepdims=True)
            t = jnp.sum(t, axis=0, keepdims=True)
            for h in range(2):
                here = (p, pl.ds(2 * n + h, 1), slice(None))
                part = slice(128 * h, 128 * (h + 1))
                m_ref[here] = jnp.minimum(m_ref[here], m[:, part])
                s_ref[here] = s_ref[here] + s[:, part]
                t_ref[here] = t_ref[here] + t[:, part]
        return carry

    lax.fori_loop(0, total, slot, 0)

    m = m_ref[...].reshape(64, 128)
    seen = m < 0.5 * UNSEEN
    unsafe = jnp.max(jnp.where(seen & (m > SAFE), 1.0, 0.0)) > 0.0
    back = jnp.exp2(jnp.where(seen, m, OFFSET) - OFFSET)
    out[0:64, :] = jnp.where(seen, m, FAR)
    out[64:128, :] = s_ref[...].reshape(64, 128) * back
    out[128:192, :] = t_ref[...].reshape(64, 128) * back

    @pl.when(unsafe)
    def _():
        m_ref[...] = jnp.full_like(m_ref, FAR)
        s_ref[...] = jnp.zeros_like(s_ref)
        t_ref[...] = jnp.zeros_like(t_ref)

        def far_slot(q, carry):
            p = block_of(q)
            load(q)
            for n in range(4):
                multiply(p, n, even)

                def terms(g):
                    rows = pl.ds(pl.multiple_of(8 * g, 8), 8)
                    more = pl.ds(pl.multiple_of(BE + 8 * g, 8), 8)
                    half = spread[rows, 0:128]
                    value = spread[rows, 128:256]
                    half = jnp.concatenate([half, half], axis=1)
                    value = jnp.concatenate([value, value], axis=1)
                    return squared_distance(even[rows, :], even[more, :], half), value

                least = lax.fori_loop(
                    0,
                    BE // 8,
                    lambda g, m: jnp.minimum(m, terms(g)[0]),
                    jnp.full((8, 256), UNSEEN, jnp.float32),
                )
                least = jnp.min(least, axis=0, keepdims=True)

                def add(g, sums):
                    d, value = terms(g)
                    w = jnp.exp2(least - d)
                    return sums[0] + w, sums[1] + w * value

                zero = jnp.zeros((8, 256), jnp.float32)
                s, t = lax.fori_loop(0, BE // 8, add, (zero, zero))
                s = jnp.sum(s, axis=0, keepdims=True)
                t = jnp.sum(t, axis=0, keepdims=True)
                for h in range(2):
                    here = (p, pl.ds(2 * n + h, 1), slice(None))
                    part = slice(128 * h, 128 * (h + 1))
                    new = (least[:, part], s[:, part], t[:, part])
                    old = (m_ref[here], s_ref[here], t_ref[here])
                    m_ref[here], s_ref[here], t_ref[here] = combine(old, new)
            return carry

        lax.fori_loop(0, total, far_slot, 0)
        out[0:64, :] = m_ref[...].reshape(64, 128)
        out[64:128, :] = s_ref[...].reshape(64, 128)
        out[128:192, :] = t_ref[...].reshape(64, 128)


def join(cycles, block_pairs, live_slots, points, table, raws):
    body = lambda *refs: join_kernel(cycles, *refs)
    bf16, f32 = jnp.bfloat16, jnp.float32
    pairs = 8.0 * len(cycles) * BP * BE
    return pl.pallas_call(
        body,
        out_shape=jax.ShapeDtypeStruct((192, 128), f32),
        in_specs=[SMEM] * 2 + [VMEM] * (2 + len(raws)),
        out_specs=VMEM,
        scratch_shapes=[
            pltpu.VMEM((len(cycles), 3 * BE, 128), bf16),
            pltpu.VMEM((8, 128, BP), bf16),
            pltpu.VMEM((128, 256), bf16),
            pltpu.VMEM((3 * BE, 128), bf16),
            pltpu.VMEM((BE, 256), f32),
            pltpu.VMEM((2 * BE, 256), f32),
            pltpu.VMEM((2 * BE, 256), f32),
            pltpu.VMEM((8, 8, 128), f32),
            pltpu.VMEM((8, 8, 128), f32),
            pltpu.VMEM((8, 8, 128), f32),
        ],
        compiler_params=pltpu.CompilerParams(vmem_limit_bytes=40 << 20),
        cost_estimate=pl.CostEstimate(
            flops=int(20 * pairs), bytes_accessed=1 << 20, transcendentals=int(pairs)
        ),
        name="join" + "".join(map(str, cycles)),
    )(block_pairs, live_slots, points, table, *raws)


def combine(one, other):
    least = jnp.minimum(one[0], other[0])
    share = jnp.exp2(least - one[0])
    other_share = jnp.exp2(least - other[0])
    return (
        least,
        one[1] * share + other[1] * other_share,
        one[2] * share + other[2] * other_share,
    )


def unpack(state):
    return state[0:64], state[64:128], state[128:192]


def local(points, segments, edge_polygon, polygon_value, block_pairs, live_slots):
    lists = []
    for cycle in (1, 2):
        lists.append(from_behind(block_pairs, "pts", -cycle))
        lists.append(from_behind(block_pairs, "pts", cycle))
    own, up1, down1, up2, down2 = pick(block_pairs, lists, segments, edge_polygon)
    lower1 = from_behind(up1, "pts", 1)
    upper1 = from_behind(down1, "pts", -1)
    lower2 = from_behind(up2, "pts", 2)
    upper2 = from_behind(down2, "pts", -2)
    table = polygon_value.reshape(-1, 128)
    first = join((0,), block_pairs, live_slots, points, table, (own, own))
    later = join((1, 2), block_pairs, live_slots, points, table, (lower1, upper1, lower2, upper2))
    mine = jnp.concatenate(combine(unpack(first), unpack(later)), axis=0)
    state = unpack(mine)
    shards = lax.axis_size("poly")
    for by in range(1, shards):
        theirs = lax.ppermute(mine, "poly", [(i, (i + by) % shards) for i in range(shards)])
        state = combine(state, unpack(theirs))
    state = combine(state, (FAR, 1.0, 0.0))
    return (state[0] * (1.0 / SCALE)).reshape(-1), (state[2] / state[1]).reshape(-1)


def solution(mesh):
    placed = (
        P(None, "pts"),
        P(None, ("pts", "poly")),
        P(("pts", "poly")),
        P(),
        P("pts", None, None, None),
        P("pts", None),
    )
    return jax.shard_map(
        local, mesh=mesh, in_specs=placed, out_specs=(P("pts"), P("pts")), check_vma=False
    )
```

```python
import math

import jax
import jax.numpy as jnp
from jax import lax
from jax.experimental import pallas as pl
from jax.experimental.pallas import tpu as pltpu
from jax.sharding import PartitionSpec as P

BP = 1024
BE = 512
EB = 64
SLOTS = 8
CUTOFF = 9.0
SCALE = 256.0 / 9.0 / math.log(2.0)
ROOT = math.sqrt(SCALE)
FAR = CUTOFF * SCALE
OFFSET = 110.0
SAFE = 200.0
UNSEEN = 1.0e30

SMEM = pl.BlockSpec(memory_space=pltpu.SMEM)
VMEM = pl.BlockSpec(memory_space=pltpu.VMEM)


def swapped(shard, axis, partner):
    devices = lax.axis_size(axis)
    pairs = [(i, partner(i)) for i in range(devices) if 0 <= partner(i) < devices]
    return lax.ppermute(shard, axis, pairs)


def packed_cell(segments, edge_polygon):
    corners = segments.reshape(4, -1, 128).transpose(1, 0, 2).reshape(-1, 128)
    polygons = edge_polygon.reshape(-1, 128).astype(jnp.float32)
    return jnp.concatenate([corners, polygons], axis=0)


def pieces(x):
    first = x.astype(jnp.bfloat16).astype(jnp.float32)
    rest = x - first
    second = rest.astype(jnp.bfloat16).astype(jnp.float32)
    return first, second, rest - second


def affine_rows(x_factor, y_factor, constant):
    x, y, c = pieces(x_factor), pieces(y_factor), pieces(constant)
    zero = jnp.zeros_like(x_factor)
    rows = [x[0], x[0], x[1], x[1], x[0], x[2], y[0], y[0], y[1], y[1], y[0], y[2], c[0], c[1], c[2], zero]
    return jnp.concatenate(rows, axis=0)


def look_up(table, indices):
    high = indices >> 7
    low = indices & 127
    tiles = BE // 128
    lows = [low[:, 128 * j : 128 * (j + 1)] for j in range(tiles)]
    highs = [high[:, 128 * j : 128 * (j + 1)] for j in range(tiles)]
    unroll = 32

    def step(i, found):
        for k in range(unroll):
            r = i * unroll + k
            row = jnp.broadcast_to(table[pl.ds(r, 1), :], (8, 128))
            found = tuple(
                jnp.where(
                    highs[j] == r,
                    jnp.take_along_axis(row, lows[j], axis=1, mode="promise_in_bounds"),
                    found[j],
                )
                for j in range(tiles)
            )
        return found

    start = tuple(jnp.zeros((8, 128), jnp.float32) for _ in range(tiles))
    found = lax.fori_loop(0, table.shape[0] // unroll, step, start)
    return jnp.concatenate(found, axis=1)


def prepare(raw, table, centre_x, left):
    value = look_up(table, raw[4].astype(jnp.int32))
    start_x, start_y = raw[0], raw[1]
    delta_x = raw[2] - start_x
    delta_y = raw[3] - start_y
    middle_x = (start_x - centre_x) + 0.5 * delta_x
    middle_y = (start_y - 0.5) + 0.5 * delta_y
    squared = jnp.maximum(delta_x * delta_x + delta_y * delta_y, 1e-12)
    inverse = lax.rsqrt(squared) * ROOT
    along_x = delta_x * inverse
    along_y = delta_y * inverse
    half = 0.5 * squared * inverse
    parts = (
        affine_rows(along_x, along_y, -(middle_x * along_x + middle_y * along_y)),
        affine_rows(-along_y, along_x, middle_x * along_y - middle_y * along_x),
        jnp.concatenate(
            list(pieces(half) + pieces(value)) + [jnp.zeros_like(half)] * 10, axis=0
        ),
    )
    for i, part in enumerate(parts):
        left[pl.ds(i * BE, BE), :] = part.T.astype(jnp.bfloat16)


def fill_right(points, centre_x, right, right_const):
    ones = jnp.ones((1, BP), jnp.float32)
    for p in range(8):
        px = pieces(points[0:1, p * BP : (p + 1) * BP] - centre_x)
        py = pieces(points[1:2, p * BP : (p + 1) * BP] - 0.5)
        rows = []
        for q in (px, py):
            rows += [q[0], q[1], q[0], q[1], q[2], q[0]]
        rows += [ones, ones, ones, jnp.zeros_like(ones)]
        full = jnp.concatenate([jnp.broadcast_to(r, (8, BP)) for r in rows], axis=0)
        right[p] = full.astype(jnp.bfloat16)
    row = lax.broadcasted_iota(jnp.int32, (128, 256), 0) // 8
    lane = lax.broadcasted_iota(jnp.int32, (128, 256), 1)
    first = jnp.where(lane < 128, 0, 3)
    const = jnp.where((row >= first) & (row < first + 3), 1.0, 0.0)
    right_const[...] = const.astype(jnp.bfloat16)


def squared_distance(u, v, half):
    beyond = u - jnp.minimum(jnp.maximum(u, -half), half)
    return v * v + beyond * beyond


def join_kernel(cycle, cell, pairs, live, points, table, *refs):
    if cycle == 0:
        (near, out), scratch = refs[:2], refs[2:]
    else:
        (near, far, prior, out), scratch = refs[:4], refs[4:]
    raw, left, right, right_const, masked, spread, even, odd, m_ref, s_ref, t_ref = scratch
    for s in range(SLOTS):
        name = pairs[0, cycle, 1, s]
        block = name & (EB - 1)
        if cycle:
            below_is_near = ((cell[0] >> (cycle - 1)) & 1) == 1
            take_near = (name < EB) == below_is_near

        def row(r):
            got = near[pl.ds(r, 1), :]
            return jnp.where(take_near, got, far[pl.ds(r, 1), :]) if cycle else got

        for j in range(BE // 128):
            here = pl.ds(128 * j, 128)
            for c in range(4):
                raw[c, pl.ds(s, 1), here] = row(16 * block + 4 * j + c)
            raw[4, pl.ds(s, 1), here] = row(1024 + 4 * block + j)
    centre_x = points[0:1, 0:1]
    fill_right(points, centre_x, right, right_const)
    prepare(raw, table, centre_x, left)
    m_ref[...] = jnp.full_like(m_ref, UNSEEN)
    s_ref[...] = jnp.zeros_like(s_ref)
    t_ref[...] = jnp.zeros_like(t_ref)

    total = live[0, cycle]
    lane = lax.broadcasted_iota(jnp.int32, (1, 128), 1) & 7
    bufs = (even, odd)

    def load(q):
        mask = (lane == q).astype(jnp.bfloat16)
        masked[...] = left[...] * mask
        spread[...] = jnp.dot(
            masked[2 * BE :, :], right_const[...], preferred_element_type=jnp.float32
        )

    def block_of(q):
        return pairs[0, cycle, 0, q]

    def multiply(p, n, buf):
        buf[...] = jnp.dot(
            masked[: 2 * BE, :],
            right[p, :, 256 * n : 256 * (n + 1)],
            preferred_element_type=jnp.float32,
        )

    def slot(q, carry):
        p = block_of(q)
        load(q)
        multiply(p, 0, even)
        for n in range(4):
            if n < 3:
                multiply(p, n + 1, bufs[(n + 1) % 2])
            buf = bufs[n % 2]
            m = s = t = None
            for g in range(BE // 8):
                half = spread[8 * g : 8 * g + 8, 0:128]
                value = spread[8 * g : 8 * g + 8, 128:256]
                half = jnp.concatenate([half, half], axis=1)
                value = jnp.concatenate([value, value], axis=1)
                d = squared_distance(
                    buf[8 * g : 8 * g + 8, :], buf[BE + 8 * g : BE + 8 * g + 8, :], half
                )
                w = jnp.exp2(OFFSET - d)
                m = d if m is None else jnp.minimum(m, d)
                s = w if s is None else s + w
                t = w * value if t is None else t + w * value
            m = jnp.min(m, axis=0, keepdims=True)
            s = jnp.sum(s, axis=0, keepdims=True)
            t = jnp.sum(t, axis=0, keepdims=True)
            for h in range(2):
                here = (p, pl.ds(2 * n + h, 1), slice(None))
                part = slice(128 * h, 128 * (h + 1))
                m_ref[here] = jnp.minimum(m_ref[here], m[:, part])
                s_ref[here] = s_ref[here] + s[:, part]
                t_ref[here] = t_ref[here] + t[:, part]
        return carry

    lax.fori_loop(0, total, slot, 0)

    m = m_ref[...].reshape(64, 128)
    seen = m < 0.5 * UNSEEN
    unsafe = jnp.max(jnp.where(seen & (m > SAFE), 1.0, 0.0)) > 0.0
    back = jnp.exp2(jnp.where(seen, m, OFFSET) - OFFSET)

    def finish(*state):
        if cycle:
            state = combine(state, unpack(prior))
        for i, part in enumerate(state):
            out[64 * i : 64 * (i + 1), :] = part

    s = s_ref[...].reshape(64, 128) * back
    t = t_ref[...].reshape(64, 128) * back
    finish(jnp.where(seen, m, FAR), s, t)

    @pl.when(unsafe)
    def _():
        m_ref[...] = jnp.full_like(m_ref, FAR)
        s_ref[...] = jnp.zeros_like(s_ref)
        t_ref[...] = jnp.zeros_like(t_ref)

        def far_slot(q, carry):
            p = block_of(q)
            load(q)
            for n in range(4):
                multiply(p, n, even)

                def terms(g):
                    rows = pl.ds(pl.multiple_of(8 * g, 8), 8)
                    more = pl.ds(pl.multiple_of(BE + 8 * g, 8), 8)
                    half = spread[rows, 0:128]
                    value = spread[rows, 128:256]
                    half = jnp.concatenate([half, half], axis=1)
                    value = jnp.concatenate([value, value], axis=1)
                    return squared_distance(even[rows, :], even[more, :], half), value

                least = lax.fori_loop(
                    0,
                    BE // 8,
                    lambda g, m: jnp.minimum(m, terms(g)[0]),
                    jnp.full((8, 256), UNSEEN, jnp.float32),
                )
                least = jnp.min(least, axis=0, keepdims=True)

                def add(g, sums):
                    d, value = terms(g)
                    w = jnp.exp2(least - d)
                    return sums[0] + w, sums[1] + w * value

                zero = jnp.zeros((8, 256), jnp.float32)
                s, t = lax.fori_loop(0, BE // 8, add, (zero, zero))
                s = jnp.sum(s, axis=0, keepdims=True)
                t = jnp.sum(t, axis=0, keepdims=True)
                for h in range(2):
                    here = (p, pl.ds(2 * n + h, 1), slice(None))
                    part = slice(128 * h, 128 * (h + 1))
                    new = (least[:, part], s[:, part], t[:, part])
                    old = (m_ref[here], s_ref[here], t_ref[here])
                    m_ref[here], s_ref[here], t_ref[here] = combine(old, new)
            return carry

        lax.fori_loop(0, total, far_slot, 0)
        finish(*(ref[...].reshape(64, 128) for ref in (m_ref, s_ref, t_ref)))


def join(cycle, cell, block_pairs, live_slots, points, table, *sources):
    body = lambda *refs: join_kernel(cycle, *refs)
    bf16, f32 = jnp.bfloat16, jnp.float32
    pairs = 8.0 * BP * BE
    return pl.pallas_call(
        body,
        out_shape=jax.ShapeDtypeStruct((192, 128), f32),
        in_specs=[SMEM] * 3 + [VMEM] * (2 + len(sources)),
        out_specs=VMEM,
        scratch_shapes=[
            pltpu.VMEM((5, SLOTS, BE), f32),
            pltpu.VMEM((3 * BE, 128), bf16),
            pltpu.VMEM((8, 128, BP), bf16),
            pltpu.VMEM((128, 256), bf16),
            pltpu.VMEM((3 * BE, 128), bf16),
            pltpu.VMEM((BE, 256), f32),
            pltpu.VMEM((2 * BE, 256), f32),
            pltpu.VMEM((2 * BE, 256), f32),
            pltpu.VMEM((8, 8, 128), f32),
            pltpu.VMEM((8, 8, 128), f32),
            pltpu.VMEM((8, 8, 128), f32),
        ],
        compiler_params=pltpu.CompilerParams(vmem_limit_bytes=40 << 20),
        cost_estimate=pl.CostEstimate(
            flops=int(20 * pairs), bytes_accessed=1 << 20, transcendentals=int(pairs)
        ),
        name="join%d" % cycle,
    )(cell, block_pairs, live_slots, points, table, *sources)


def combine(one, other):
    least = jnp.minimum(one[0], other[0])
    share = jnp.exp2(least - one[0])
    other_share = jnp.exp2(least - other[0])
    return (
        least,
        one[1] * share + other[1] * other_share,
        one[2] * share + other[2] * other_share,
    )


def unpack(state):
    return state[0:64, :], state[64:128, :], state[128:192, :]


def local(points, segments, edge_polygon, polygon_value, block_pairs, live_slots):
    mine = packed_cell(segments, edge_polygon)
    near1 = swapped(mine, "pts", lambda c: c ^ 1)
    far1 = swapped(mine, "pts", lambda c: ((c + 1) ^ 1) - 1)
    near2 = swapped(mine, "pts", lambda c: c ^ 2)
    far2 = swapped(mine, "pts", lambda c: ((c + 2) ^ 2) - 2)
    cell = lax.axis_index("pts").astype(jnp.int32).reshape(1)
    table = polygon_value.reshape(-1, 128)
    args = (cell, block_pairs, live_slots, points, table)
    part = join(0, *args, mine)
    part = join(1, *args, near1, far1, part)
    part = join(2, *args, near2, far2, part)
    state = unpack(part)
    for flip in (1, 3, 2):
        state = combine(state, unpack(swapped(part, "poly", lambda q: q ^ flip)))
    state = combine(state, (FAR, 1.0, 0.0))
    return (state[0] * (1.0 / SCALE)).reshape(-1), (state[2] / state[1]).reshape(-1)


def solution(mesh):
    placed = (
        P(None, "pts"),
        P(None, ("pts", "poly")),
        P(("pts", "poly")),
        P(),
        P("pts", None, None, None),
        P("pts", None),
    )
    return jax.shard_map(
        local, mesh=mesh, in_specs=placed, out_specs=(P("pts"), P("pts")), check_vma=False
    )
```

```python
import math

import jax
import jax.numpy as jnp
from jax import lax
from jax.experimental import pallas as pl
from jax.experimental.pallas import tpu as pltpu
from jax.sharding import PartitionSpec as P

BP = 1024
BE = 512
EB = 64
SLOTS = 8
CUTOFF = 9.0
SCALE = 256.0 / 9.0 / math.log(2.0)
ROOT = math.sqrt(SCALE)
FAR = CUTOFF * SCALE
OFFSET = 110.0
SAFE = 200.0
UNSEEN = 1.0e30

SMEM = pl.BlockSpec(memory_space=pltpu.SMEM)
VMEM = pl.BlockSpec(memory_space=pltpu.VMEM)


def swapped(shard, axis, partner):
    devices = lax.axis_size(axis)
    pairs = [(i, partner(i)) for i in range(devices) if 0 <= partner(i) < devices]
    return lax.ppermute(shard, axis, pairs)


def packed_cell(segments, edge_polygon):
    corners = segments.reshape(4, -1, 128).transpose(1, 0, 2).reshape(-1, 128)
    polygons = edge_polygon.reshape(-1, 128).astype(jnp.float32)
    return jnp.concatenate([corners, polygons], axis=0)


def pieces(x):
    first = x.astype(jnp.bfloat16).astype(jnp.float32)
    rest = x - first
    second = rest.astype(jnp.bfloat16).astype(jnp.float32)
    return first, second, rest - second


def affine_rows(x_factor, y_factor, constant):
    x, y, c = pieces(x_factor), pieces(y_factor), pieces(constant)
    zero = jnp.zeros_like(x_factor)
    rows = [x[0], x[0], x[1], x[1], x[0], x[2], y[0], y[0], y[1], y[1], y[0], y[2], c[0], c[1], c[2], zero]
    return jnp.concatenate(rows, axis=0)


def squared_distance(u, v, half):
    beyond = jnp.maximum(jnp.abs(u) - half, 0.0)
    return v * v + beyond * beyond


TILES = BE // 128


def join_kernel(cycle, pairs, live, points, table, *refs):
    if cycle == 0:
        (near, out), scratch = refs[:2], refs[2:]
    else:
        (near, far, prior, out), scratch = refs[:4], refs[4:]
    raw, names, spots, table2, halves, left, right, column, spreader = scratch[:9]
    spread, even, odd, m_ref, s_ref, t_ref = scratch[9:]
    sub8 = lax.broadcasted_iota(jnp.int32, (8, 128), 0)
    total = live[0, cycle]

    for s in range(SLOTS):
        name = pairs[0, cycle, 1, s]
        block = name & (EB - 1)
        corner_rows = pl.ds(pl.multiple_of(16 * block, 16), 16)
        name_rows = pl.ds(1024 + 4 * block, 4)
        corner, polygon = near[corner_rows, :], near[name_rows, :]
        if cycle:
            below_is_near = ((lax.axis_index("pts") >> (cycle - 1)) & 1) == 1
            take_near = (name < EB) == below_is_near
            corner = jnp.where(take_near, corner, far[corner_rows, :])
            polygon = jnp.where(take_near, polygon, far[name_rows, :])
        raw[16 * s : 16 * s + 16, :] = corner
        names[8 * s : 8 * s + 4, :] = polygon
        names[8 * s + 4 : 8 * s + 8, :] = polygon

    for r in range(128):
        one = jnp.broadcast_to(table[r : r + 1, :], (8, 128))
        other = jnp.broadcast_to(table[r + 128 : r + 129, :], (8, 128))
        table2[8 * r : 8 * r + 8, :] = jnp.where(sub8 < 4, one, other)

    for i in range(64):
        for c in range(2):
            spots[3 * c, i : i + 1, :] = points[c : c + 1, 128 * i : 128 * (i + 1)]
    centre_x = points[0:1, 0:1]
    for c, centre in ((0, centre_x), (1, 0.5)):
        for i, piece in enumerate(pieces(spots[3 * c] - centre)):
            spots[3 * c + i] = piece

    for j in range(TILES):
        start_x, start_y, end_x, end_y = (
            raw[pl.ds(4 * j + c, SLOTS, stride=16), :] for c in range(4)
        )
        delta_x = end_x - start_x
        delta_y = end_y - start_y
        middle_x = (start_x - centre_x) + 0.5 * delta_x
        middle_y = (start_y - 0.5) + 0.5 * delta_y
        squared = jnp.maximum(delta_x * delta_x + delta_y * delta_y, 1e-12)
        inverse = lax.rsqrt(squared) * ROOT
        along_x = delta_x * inverse
        along_y = delta_y * inverse
        halves[8 * j : 8 * j + 8, :] = 0.5 * squared * inverse
        along = affine_rows(along_x, along_y, -(middle_x * along_x + middle_y * along_y))
        across = affine_rows(-along_y, along_x, middle_x * along_y - middle_y * along_x)
        left[128 * j : 128 * (j + 1), :] = along.T.astype(jnp.bfloat16)
        left[BE + 128 * j : BE + 128 * (j + 1), :] = across.T.astype(jnp.bfloat16)

    row = lax.broadcasted_iota(jnp.int32, (128, 256), 0)
    lane = lax.broadcasted_iota(jnp.int32, (128, 256), 1)
    first = jnp.where(lane < 128, 24, 0)
    for j in range(TILES):
        inside = (row >= first) & (row < first + 24) & ((row & 7) == j)
        spreader[j] = jnp.where(inside, 1.0, 0.0).astype(jnp.bfloat16)

    m_ref[...] = jnp.full_like(m_ref, UNSEEN)
    s_ref[...] = jnp.zeros_like(s_ref)
    t_ref[...] = jnp.zeros_like(t_ref)

    def block_of(q):
        return pairs[0, cycle, 0, q]

    def look_up(q):
        index = names[pl.ds(pl.multiple_of(8 * q, 8), 8), :].astype(jnp.int32)
        low = index & 127
        high = index >> 7
        bits = [((high >> b) & 1) == 1 for b in range(7)]

        def found(r, b):
            if b < 0:
                part = table2[8 * r : 8 * r + 8, :]
                return jnp.take_along_axis(part, low, axis=1, mode="promise_in_bounds")
            return jnp.where(bits[b], found(r + (1 << b), b - 1), found(r, b - 1))

        both = found(0, 6)
        return jnp.where(high >= 128, pltpu.roll(both, 4, 0), both)

    def set_right(q):
        p = block_of(q)
        here = sub8 == q
        zero = jnp.zeros((8, 128), jnp.float32)
        one = jnp.where(here, 1.0, 0.0)
        for n in range(8):
            at = pl.ds(8 * p + n, 1)
            part = [
                jnp.where(here, jnp.broadcast_to(spots[i, at, :], (8, 128)), 0.0) for i in range(6)
            ]
            x, y = part[:3], part[3:]
            rows = []
            for c in (x, y):
                rows += [c[0], c[1], c[0], c[1], c[2], c[0]]
            rows += [one, one, one, zero]
            right[:, 128 * n : 128 * (n + 1)] = jnp.concatenate(rows, axis=0).astype(jnp.bfloat16)

    def set_column(q):
        half = jnp.concatenate(
            [halves[pl.ds(8 * j + q, 1), :] for j in range(TILES)]
            + [jnp.zeros((8 - TILES, 128), jnp.float32)],
            axis=0,
        )
        rows = list(pieces(look_up(q))) + list(pieces(half))
        full = jnp.concatenate(rows + [jnp.zeros((80, 128), jnp.float32)], axis=0)
        column[...] = full.T.astype(jnp.bfloat16)

    def multiply(n, buf):
        buf[...] = jnp.dot(
            left[...], right[:, 256 * n : 256 * (n + 1)], preferred_element_type=jnp.float32
        )

    def set_spread():
        for j in range(TILES):
            spread[128 * j : 128 * (j + 1), :] = jnp.dot(
                column[...], spreader[j], preferred_element_type=jnp.float32
            )

    def add_up(p, n, buf):
        m, s, t = [None, None], [None, None], [None, None]
        for g in range(BE // 8):
            up, down = slice(8 * g, 8 * g + 8), slice(BE + 8 * g, BE + 8 * g + 8)
            half = spread[up, 0:128]
            value = spread[up, 128:256]
            for h in range(2):
                at = slice(128 * h, 128 * (h + 1))
                d = squared_distance(buf[up, at], buf[down, at], half)
                w = jnp.exp2(OFFSET - d)
                m[h] = jnp.minimum(m[h], d) if g else d
                s[h] = s[h] + w if g else w
                t[h] = t[h] + w * value if g else w * value
        for h in range(2):
            here = pl.ds(8 * p + (2 * n + h), 1)
            m_ref[here, :] = jnp.minimum(m_ref[here, :], jnp.min(m[h], axis=0, keepdims=True))
            s_ref[here, :] = s_ref[here, :] + jnp.sum(s[h], axis=0, keepdims=True)
            t_ref[here, :] = t_ref[here, :] + jnp.sum(t[h], axis=0, keepdims=True)

    set_right(0)
    multiply(0, even)
    set_column(0)
    set_spread()

    def slot(q, carry):
        p = block_of(q)
        later = jnp.minimum(q + 1, total - 1)
        multiply(1, odd)
        add_up(p, 0, even)
        multiply(2, even)
        add_up(p, 1, odd)
        multiply(3, odd)
        add_up(p, 2, even)
        set_right(later)
        set_column(later)
        multiply(0, even)
        add_up(p, 3, odd)
        set_spread()
        return carry

    lax.fori_loop(0, total, slot, 0)

    def finish(*result):
        if cycle:
            result = combine(result, unpack(prior))
        for i, part in enumerate(result):
            out[64 * i : 64 * (i + 1), :] = part

    m = m_ref[...]
    seen = m < 0.5 * UNSEEN
    unsafe = jnp.max(jnp.where(seen & (m > SAFE), 1.0, 0.0)) > 0.0
    back = jnp.exp2(jnp.where(seen, m, OFFSET) - OFFSET)
    finish(jnp.where(seen, m, FAR), s_ref[...] * back, t_ref[...] * back)

    @pl.when(unsafe)
    def _():
        m_ref[...] = jnp.full_like(m_ref, FAR)
        s_ref[...] = jnp.zeros_like(s_ref)
        t_ref[...] = jnp.zeros_like(t_ref)

        def far_slot(q, carry):
            set_right(q)
            set_column(q)
            set_spread()
            for n in range(4):
                multiply(n, even)
                for h in range(2):
                    at = slice(128 * h, 128 * (h + 1))

                    def terms(g):
                        up = pl.ds(pl.multiple_of(8 * g, 8), 8)
                        down = pl.ds(pl.multiple_of(BE + 8 * g, 8), 8)
                        d = squared_distance(even[up, at], even[down, at], spread[up, 0:128])
                        return d, spread[up, 128:256]

                    def lower(g, m):
                        return jnp.minimum(m, terms(g)[0])

                    least = jnp.full((8, 128), UNSEEN, jnp.float32)
                    least = lax.fori_loop(0, BE // 8, lower, least)
                    least = jnp.min(least, axis=0, keepdims=True)

                    def add(g, sums):
                        d, value = terms(g)
                        w = jnp.exp2(least - d)
                        return sums[0] + w, sums[1] + w * value

                    zero = jnp.zeros((8, 128), jnp.float32)
                    sums = lax.fori_loop(0, BE // 8, add, (zero, zero))
                    new = (least, *(jnp.sum(x, axis=0, keepdims=True) for x in sums))
                    here = pl.ds(8 * block_of(q) + (2 * n + h), 1)
                    old = (m_ref[here, :], s_ref[here, :], t_ref[here, :])
                    m_ref[here, :], s_ref[here, :], t_ref[here, :] = combine(old, new)
            return carry

        lax.fori_loop(0, total, far_slot, 0)
        finish(m_ref[...], s_ref[...], t_ref[...])


def join(cycle, block_pairs, live_slots, points, table, *sources):
    body = lambda *refs: join_kernel(cycle, *refs)
    bf16, f32 = jnp.bfloat16, jnp.float32
    pairs = 8.0 * BP * BE
    return pl.pallas_call(
        body,
        out_shape=jax.ShapeDtypeStruct((192, 128), f32),
        in_specs=[SMEM] * 2 + [VMEM] * (2 + len(sources)),
        out_specs=VMEM,
        scratch_shapes=[
            pltpu.VMEM((16 * SLOTS, 128), f32),
            pltpu.VMEM((8 * SLOTS, 128), f32),
            pltpu.VMEM((6, 64, 128), f32),
            pltpu.VMEM((1024, 128), f32),
            pltpu.VMEM((32, 128), f32),
            pltpu.VMEM((2 * BE, 128), bf16),
            pltpu.VMEM((128, BP), bf16),
            pltpu.VMEM((128, 128), bf16),
            pltpu.VMEM((TILES, 128, 256), bf16),
        ]
        + [pltpu.VMEM((BE, 256), f32)]
        + [pltpu.VMEM((2 * BE, 256), f32)] * 2
        + [pltpu.VMEM((64, 128), f32)] * 3,
        compiler_params=pltpu.CompilerParams(vmem_limit_bytes=40 << 20),
        cost_estimate=pl.CostEstimate(
            flops=int(20 * pairs), bytes_accessed=1 << 20, transcendentals=int(pairs)
        ),
        name="join%d" % cycle,
    )(block_pairs, live_slots, points, table, *sources)


def combine(one, other):
    least = jnp.minimum(one[0], other[0])
    share = jnp.exp2(least - one[0])
    other_share = jnp.exp2(least - other[0])
    return (
        least,
        one[1] * share + other[1] * other_share,
        one[2] * share + other[2] * other_share,
    )


def unpack(state):
    return state[0:64, :], state[64:128, :], state[128:192, :]


def local(points, segments, edge_polygon, polygon_value, block_pairs, live_slots):
    mine = packed_cell(segments, edge_polygon)
    near1 = swapped(mine, "pts", lambda c: c ^ 1)
    far1 = swapped(mine, "pts", lambda c: ((c + 1) ^ 1) - 1)
    near2 = swapped(mine, "pts", lambda c: c ^ 2)
    far2 = swapped(mine, "pts", lambda c: ((c + 2) ^ 2) - 2)
    table = polygon_value.reshape(-1, 128)
    args = (block_pairs, live_slots, points, table)
    part = join(0, *args, mine)
    part = join(1, *args, near1, far1, part)
    part = join(2, *args, near2, far2, part)
    state = unpack(part)
    for flip in (1, 3, 2):
        state = combine(state, unpack(swapped(part, "poly", lambda q: q ^ flip)))
    state = combine(state, (FAR, 1.0, 0.0))
    return (state[0] * (1.0 / SCALE)).reshape(-1), (state[2] / state[1]).reshape(-1)


def solution(mesh):
    placed = (
        P(None, "pts"),
        P(None, ("pts", "poly")),
        P(("pts", "poly")),
        P(),
        P("pts", None, None, None),
        P("pts", None),
    )
    return jax.shard_map(
        local, mesh=mesh, in_specs=placed, out_specs=(P("pts"), P("pts")), check_vma=False
    )
```

```python
import math

import jax
import jax.numpy as jnp
from jax import lax
from jax.experimental import pallas as pl
from jax.experimental.pallas import tpu as pltpu
from jax.sharding import PartitionSpec as P


BP = 1024
BE = 512
EB = 64
SLOTS = 8
CUTOFF = 9.0
SCALE = 256.0 / 9.0 / math.log(2.0)
ROOT = math.sqrt(SCALE)
FAR = CUTOFF * SCALE
OFFSET = 110.0
SAFE = 200.0
UNSEEN = 1.0e30

SMEM = pl.BlockSpec(memory_space=pltpu.SMEM)
VMEM = pl.BlockSpec(memory_space=pltpu.VMEM)


def swapped(shard, axis, partner):
    devices = lax.axis_size(axis)
    pairs = [(i, partner(i)) for i in range(devices) if 0 <= partner(i) < devices]
    return lax.ppermute(shard, axis, pairs)


def pack_kernel(corners, polygons, out):
    out[0:1024, :] = corners[...]
    out[1024:1280, :] = polygons[...].astype(jnp.float32)


def packed_cell(segments, edge_polygon):
    corners = segments.reshape(4, -1, 128).transpose(1, 0, 2).reshape(-1, 128)
    return pl.pallas_call(
        pack_kernel,
        out_shape=jax.ShapeDtypeStruct((1280, 128), jnp.float32),
        in_specs=[VMEM] * 2,
        out_specs=VMEM,
        compiler_params=pltpu.CompilerParams(vmem_limit_bytes=4 << 20),
        cost_estimate=pl.CostEstimate(flops=1 << 20, bytes_accessed=1 << 21, transcendentals=0),
        name="pack",
    )(corners, edge_polygon.reshape(-1, 128))


def pieces(x):
    first = x.astype(jnp.bfloat16).astype(jnp.float32)
    rest = x - first
    second = rest.astype(jnp.bfloat16).astype(jnp.float32)
    return first, second, rest - second


def affine_rows(x_factor, y_factor, constant):
    x, y, c = pieces(x_factor), pieces(y_factor), pieces(constant)
    zero = jnp.zeros_like(x_factor)
    rows = [x[0], x[0], x[1], x[1], x[0], x[2], y[0], y[0], y[1], y[1], y[0], y[2], c[0], c[1], c[2], zero]
    return jnp.concatenate(rows, axis=0)


def squared_distance(u, v, half):
    beyond = jnp.maximum(jnp.abs(u) - half, 0.0)
    return v * v + beyond * beyond


TILES = BE // 128


def join_kernel(cycle, pairs, live, points, table, *refs):
    if cycle == 0:
        (near, out), scratch = refs[:2], refs[2:]
    else:
        (near, far, prior, out), scratch = refs[:4], refs[4:]
    raw, names, spots, table2, halves, left, right, column, spreader = scratch[:9]
    spread, even, odd, m_ref, s_ref, t_ref = scratch[9:]
    sub8 = lax.broadcasted_iota(jnp.int32, (8, 128), 0)
    total = live[0, cycle]

    for s in range(SLOTS):
        name = pairs[0, cycle, 1, s]
        block = name & (EB - 1)
        corner_rows = pl.ds(pl.multiple_of(16 * block, 16), 16)
        name_rows = pl.ds(1024 + 4 * block, 4)
        corner, polygon = near[corner_rows, :], near[name_rows, :]
        if cycle:
            below_is_near = (lax.axis_index("pts") & 1) == 1
            take_near = (name < EB) == below_is_near
            corner = jnp.where(take_near, corner, far[corner_rows, :])
            polygon = jnp.where(take_near, polygon, far[name_rows, :])
        raw[16 * s : 16 * s + 16, :] = corner
        names[8 * s : 8 * s + 4, :] = polygon
        names[8 * s + 4 : 8 * s + 8, :] = polygon

    for r in range(128):
        one = jnp.broadcast_to(table[r : r + 1, :], (8, 128))
        other = jnp.broadcast_to(table[r + 128 : r + 129, :], (8, 128))
        table2[8 * r : 8 * r + 8, :] = jnp.where(sub8 < 4, one, other)

    for i in range(64):
        for c in range(2):
            spots[3 * c, i : i + 1, :] = points[c : c + 1, 128 * i : 128 * (i + 1)]
    centre_x = points[0:1, 0:1]
    for c, centre in ((0, centre_x), (1, 0.5)):
        for i, piece in enumerate(pieces(spots[3 * c] - centre)):
            spots[3 * c + i] = piece

    for j in range(TILES):
        start_x, start_y, end_x, end_y = (
            raw[pl.ds(4 * j + c, SLOTS, stride=16), :] for c in range(4)
        )
        delta_x = end_x - start_x
        delta_y = end_y - start_y
        middle_x = (start_x - centre_x) + 0.5 * delta_x
        middle_y = (start_y - 0.5) + 0.5 * delta_y
        squared = jnp.maximum(delta_x * delta_x + delta_y * delta_y, 1e-12)
        inverse = lax.rsqrt(squared) * ROOT
        along_x = delta_x * inverse
        along_y = delta_y * inverse
        halves[8 * j : 8 * j + 8, :] = 0.5 * squared * inverse
        along = affine_rows(along_x, along_y, -(middle_x * along_x + middle_y * along_y))
        across = affine_rows(-along_y, along_x, middle_x * along_y - middle_y * along_x)
        left[128 * j : 128 * (j + 1), :] = along.T.astype(jnp.bfloat16)
        left[BE + 128 * j : BE + 128 * (j + 1), :] = across.T.astype(jnp.bfloat16)

    row = lax.broadcasted_iota(jnp.int32, (128, 256), 0)
    lane = lax.broadcasted_iota(jnp.int32, (128, 256), 1)
    first = jnp.where(lane < 128, 24, 0)
    for j in range(TILES):
        inside = (row >= first) & (row < first + 24) & ((row & 7) == j)
        spreader[j] = jnp.where(inside, 1.0, 0.0).astype(jnp.bfloat16)

    m_ref[...] = jnp.full_like(m_ref, UNSEEN)
    s_ref[...] = jnp.zeros_like(s_ref)
    t_ref[...] = jnp.zeros_like(t_ref)

    def block_of(q):
        return pairs[0, cycle, 0, q]

    def look_up(q):
        index = names[pl.ds(pl.multiple_of(8 * q, 8), 8), :].astype(jnp.int32)
        low = index & 127
        high = index >> 7
        bits = [((high >> b) & 1) == 1 for b in range(7)]

        def found(r, b):
            if b < 0:
                part = table2[8 * r : 8 * r + 8, :]
                return jnp.take_along_axis(part, low, axis=1, mode="promise_in_bounds")
            return jnp.where(bits[b], found(r + (1 << b), b - 1), found(r, b - 1))

        both = found(0, 6)
        return jnp.where(high >= 128, pltpu.roll(both, 4, 0), both)

    def set_right(q):
        p = block_of(q)
        here = sub8 == q
        zero = jnp.zeros((8, 128), jnp.float32)
        one = jnp.where(here, 1.0, 0.0)
        for n in range(8):
            at = pl.ds(8 * p + n, 1)
            part = [
                jnp.where(here, jnp.broadcast_to(spots[i, at, :], (8, 128)), 0.0) for i in range(6)
            ]
            x, y = part[:3], part[3:]
            rows = []
            for c in (x, y):
                rows += [c[0], c[1], c[0], c[1], c[2], c[0]]
            rows += [one, one, one, zero]
            right[:, 128 * n : 128 * (n + 1)] = jnp.concatenate(rows, axis=0).astype(jnp.bfloat16)

    def set_column(q):
        half = jnp.concatenate(
            [halves[pl.ds(8 * j + q, 1), :] for j in range(TILES)]
            + [jnp.zeros((8 - TILES, 128), jnp.float32)],
            axis=0,
        )
        rows = list(pieces(look_up(q))) + list(pieces(half))
        full = jnp.concatenate(rows + [jnp.zeros((80, 128), jnp.float32)], axis=0)
        column[...] = full.T.astype(jnp.bfloat16)

    def multiply(n, buf):
        buf[...] = jnp.dot(
            left[...], right[:, 256 * n : 256 * (n + 1)], preferred_element_type=jnp.float32
        )

    def set_spread():
        for j in range(TILES):
            spread[128 * j : 128 * (j + 1), :] = jnp.dot(
                column[...], spreader[j], preferred_element_type=jnp.float32
            )

    def add_up(p, n, buf):
        m, s, t = [None, None], [None, None], [None, None]
        for g in range(BE // 8):
            up, down = slice(8 * g, 8 * g + 8), slice(BE + 8 * g, BE + 8 * g + 8)
            half = spread[up, 0:128]
            value = spread[up, 128:256]
            for h in range(2):
                at = slice(128 * h, 128 * (h + 1))
                d = squared_distance(buf[up, at], buf[down, at], half)
                w = jnp.exp2(OFFSET - d)
                m[h] = jnp.minimum(m[h], d) if g else d
                s[h] = s[h] + w if g else w
                t[h] = t[h] + w * value if g else w * value
        for h in range(2):
            here = pl.ds(8 * p + (2 * n + h), 1)
            m_ref[here, :] = jnp.minimum(m_ref[here, :], jnp.min(m[h], axis=0, keepdims=True))
            s_ref[here, :] = s_ref[here, :] + jnp.sum(s[h], axis=0, keepdims=True)
            t_ref[here, :] = t_ref[here, :] + jnp.sum(t[h], axis=0, keepdims=True)

    set_right(0)
    multiply(0, even)
    set_column(0)
    set_spread()

    def slot(q, carry):
        p = block_of(q)
        later = jnp.minimum(q + 1, total - 1)
        multiply(1, odd)
        add_up(p, 0, even)
        multiply(2, even)
        add_up(p, 1, odd)
        multiply(3, odd)
        add_up(p, 2, even)
        set_right(later)
        set_column(later)
        multiply(0, even)
        add_up(p, 3, odd)
        set_spread()
        return carry

    lax.fori_loop(0, total, slot, 0)

    def finish(*result):
        if cycle:
            result = combine(result, unpack(prior))
        for i, part in enumerate(result):
            out[64 * i : 64 * (i + 1), :] = part

    m = m_ref[...]
    seen = m < 0.5 * UNSEEN
    unsafe = jnp.max(jnp.where(seen & (m > SAFE), 1.0, 0.0)) > 0.0
    back = jnp.exp2(jnp.where(seen, m, OFFSET) - OFFSET)
    finish(jnp.where(seen, m, FAR), s_ref[...] * back, t_ref[...] * back)

    @pl.when(unsafe)
    def _():
        m_ref[...] = jnp.full_like(m_ref, FAR)
        s_ref[...] = jnp.zeros_like(s_ref)
        t_ref[...] = jnp.zeros_like(t_ref)

        def far_slot(q, carry):
            set_right(q)
            set_column(q)
            set_spread()
            for n in range(4):
                multiply(n, even)
                for h in range(2):
                    at = slice(128 * h, 128 * (h + 1))

                    def terms(g):
                        up = pl.ds(pl.multiple_of(8 * g, 8), 8)
                        down = pl.ds(pl.multiple_of(BE + 8 * g, 8), 8)
                        d = squared_distance(even[up, at], even[down, at], spread[up, 0:128])
                        return d, spread[up, 128:256]

                    def lower(g, m):
                        return jnp.minimum(m, terms(g)[0])

                    least = jnp.full((8, 128), UNSEEN, jnp.float32)
                    least = lax.fori_loop(0, BE // 8, lower, least)
                    least = jnp.min(least, axis=0, keepdims=True)

                    def add(g, sums):
                        d, value = terms(g)
                        w = jnp.exp2(least - d)
                        return sums[0] + w, sums[1] + w * value

                    zero = jnp.zeros((8, 128), jnp.float32)
                    sums = lax.fori_loop(0, BE // 8, add, (zero, zero))
                    new = (least, *(jnp.sum(x, axis=0, keepdims=True) for x in sums))
                    here = pl.ds(8 * block_of(q) + (2 * n + h), 1)
                    old = (m_ref[here, :], s_ref[here, :], t_ref[here, :])
                    m_ref[here, :], s_ref[here, :], t_ref[here, :] = combine(old, new)
            return carry

        lax.fori_loop(0, total, far_slot, 0)
        finish(m_ref[...], s_ref[...], t_ref[...])


def join(cycle, block_pairs, live_slots, points, table, *sources):
    body = lambda *refs: join_kernel(cycle, *refs)
    bf16, f32 = jnp.bfloat16, jnp.float32
    pairs = 8.0 * BP * BE
    return pl.pallas_call(
        body,
        out_shape=jax.ShapeDtypeStruct((192, 128), f32),
        in_specs=[SMEM] * 2 + [VMEM] * (2 + len(sources)),
        out_specs=VMEM,
        scratch_shapes=[
            pltpu.VMEM((16 * SLOTS, 128), f32),
            pltpu.VMEM((8 * SLOTS, 128), f32),
            pltpu.VMEM((6, 64, 128), f32),
            pltpu.VMEM((1024, 128), f32),
            pltpu.VMEM((32, 128), f32),
            pltpu.VMEM((2 * BE, 128), bf16),
            pltpu.VMEM((128, BP), bf16),
            pltpu.VMEM((128, 128), bf16),
            pltpu.VMEM((TILES, 128, 256), bf16),
        ]
        + [pltpu.VMEM((BE, 256), f32)]
        + [pltpu.VMEM((2 * BE, 256), f32)] * 2
        + [pltpu.VMEM((64, 128), f32)] * 3,
        compiler_params=pltpu.CompilerParams(vmem_limit_bytes=40 << 20),
        cost_estimate=pl.CostEstimate(
            flops=int(20 * pairs), bytes_accessed=1 << 20, transcendentals=int(pairs)
        ),
    )(block_pairs, live_slots, points, table, *sources)


def combine(one, other):
    least = jnp.minimum(one[0], other[0])
    share = jnp.exp2(least - one[0])
    other_share = jnp.exp2(least - other[0])
    return (
        least,
        one[1] * share + other[1] * other_share,
        one[2] * share + other[2] * other_share,
    )


def unpack(state):
    return state[0:64, :], state[64:128, :], state[128:192, :]


def steps(points, segments, edge_polygon, polygon_value, block_pairs, live_slots):
    mine = packed_cell(segments, edge_polygon)
    inner = lambda shard: swapped(shard, "pts", lambda c: c ^ 1)
    outer = lambda shard: swapped(shard, "pts", lambda c: ((c + 1) ^ 1) - 1)
    args = (block_pairs, live_slots, points, polygon_value.reshape(-1, 128))
    near1 = inner(mine)
    far1 = outer(mine)
    far2 = outer(near1)
    part = join(0, *args, mine)
    far1, part = lax.optimization_barrier((far1, part))
    near2 = inner(far1)
    part = join(1, *args, near1, far1, part)
    part = join(2, *args, near2, far2, part)
    state = unpack(part)
    for flip in (1, 3, 2):
        state = combine(state, unpack(swapped(part, "poly", lambda q: q ^ flip)))
    state = combine(state, (FAR, 1.0, 0.0))
    return (state[0] * (1.0 / SCALE)).reshape(-1), (state[2] / state[1]).reshape(-1)


def solution(mesh):
    placed = (
        P(None, "pts"),
        P(None, ("pts", "poly")),
        P(("pts", "poly")),
        P(),
        P("pts", None, None, None),
        P("pts", None),
    )
    return jax.shard_map(
        steps, mesh=mesh, in_specs=placed, out_specs=(P("pts"), P("pts")), check_vma=False
    )
```

```python
import math

import jax
import jax.numpy as jnp
from jax import lax
from jax.experimental import pallas as pl
from jax.experimental.pallas import tpu as pltpu
from jax.sharding import PartitionSpec as P


BP = 1024
BE = 512
EB = 64
SLOTS = 8
CUTOFF = 9.0
SCALE = 256.0 / 9.0 / math.log(2.0)
ROOT = math.sqrt(SCALE)
FAR = CUTOFF * SCALE
OFFSET = 110.0
SAFE = 200.0
UNSEEN = 1.0e30

SMEM = pl.BlockSpec(memory_space=pltpu.SMEM)
VMEM = pl.BlockSpec(memory_space=pltpu.VMEM)


def swapped(shard, axis, partner):
    devices = lax.axis_size(axis)
    pairs = [(i, partner(i)) for i in range(devices) if 0 <= partner(i) < devices]
    return lax.ppermute(shard, axis, pairs)


def pack_kernel(corners, polygons, out):
    out[0:1024, :] = corners[...]
    out[1024:1280, :] = polygons[...].astype(jnp.float32)


def packed_cell(segments, edge_polygon):
    corners = segments.reshape(4, -1, 128).transpose(1, 0, 2).reshape(-1, 128)
    return pl.pallas_call(
        pack_kernel,
        out_shape=jax.ShapeDtypeStruct((1280, 128), jnp.float32),
        in_specs=[VMEM] * 2,
        out_specs=VMEM,
        compiler_params=pltpu.CompilerParams(vmem_limit_bytes=4 << 20),
        cost_estimate=pl.CostEstimate(flops=1 << 20, bytes_accessed=1 << 21, transcendentals=0),
        name="pack",
    )(corners, edge_polygon.reshape(-1, 128))


def pieces(x):
    first = x.astype(jnp.bfloat16).astype(jnp.float32)
    rest = x - first
    second = rest.astype(jnp.bfloat16).astype(jnp.float32)
    return first, second, rest - second


def affine_rows(x_factor, y_factor, constant):
    x, y, c = pieces(x_factor), pieces(y_factor), pieces(constant)
    zero = jnp.zeros_like(x_factor)
    rows = [x[0], x[0], x[1], x[1], x[0], x[2], y[0], y[0], y[1], y[1], y[0], y[2], c[0], c[1], c[2], zero]
    return jnp.concatenate(rows, axis=0)


def squared_distance(u, v, half):
    beyond = jnp.maximum(jnp.abs(u) - half, 0.0)
    return v * v + beyond * beyond


TILES = BE // 128


def join_kernel(cycle, pairs, live, points, table, *refs):
    if cycle == 0:
        (near, out), scratch = refs[:2], refs[2:]
    else:
        (near, far, prior, out), scratch = refs[:4], refs[4:]
    raw, names, spots, table2, halves, left, right, column, spreader = scratch[:9]
    spread, even, m_ref, s_ref, t_ref = scratch[9:]
    sub8 = lax.broadcasted_iota(jnp.int32, (8, 128), 0)
    total = live[0, cycle]

    for s in range(SLOTS):
        name = pairs[0, cycle, 1, s]
        block = name & (EB - 1)
        corner_rows = pl.ds(pl.multiple_of(16 * block, 16), 16)
        name_rows = pl.ds(1024 + 4 * block, 4)
        corner, polygon = near[corner_rows, :], near[name_rows, :]
        if cycle:
            below_is_near = (lax.axis_index("pts") & 1) == 1
            take_near = (name < EB) == below_is_near
            corner = jnp.where(take_near, corner, far[corner_rows, :])
            polygon = jnp.where(take_near, polygon, far[name_rows, :])
        raw[16 * s : 16 * s + 16, :] = corner
        names[8 * s : 8 * s + 4, :] = polygon
        names[8 * s + 4 : 8 * s + 8, :] = polygon

    for r in range(128):
        one = jnp.broadcast_to(table[r : r + 1, :], (8, 128))
        other = jnp.broadcast_to(table[r + 128 : r + 129, :], (8, 128))
        table2[8 * r : 8 * r + 8, :] = jnp.where(sub8 < 4, one, other)

    for i in range(64):
        for c in range(2):
            spots[3 * c, i : i + 1, :] = points[c : c + 1, 128 * i : 128 * (i + 1)]
    centre_x = points[0:1, 0:1]
    for c, centre in ((0, centre_x), (1, 0.5)):
        for i, piece in enumerate(pieces(spots[3 * c] - centre)):
            spots[3 * c + i] = piece

    for j in range(TILES):
        start_x, start_y, end_x, end_y = (
            raw[pl.ds(4 * j + c, SLOTS, stride=16), :] for c in range(4)
        )
        delta_x = end_x - start_x
        delta_y = end_y - start_y
        middle_x = (start_x - centre_x) + 0.5 * delta_x
        middle_y = (start_y - 0.5) + 0.5 * delta_y
        squared = jnp.maximum(delta_x * delta_x + delta_y * delta_y, 1e-12)
        inverse = lax.rsqrt(squared) * ROOT
        along_x = delta_x * inverse
        along_y = delta_y * inverse
        halves[8 * j : 8 * j + 8, :] = 0.5 * squared * inverse
        along = affine_rows(along_x, along_y, -(middle_x * along_x + middle_y * along_y))
        across = affine_rows(-along_y, along_x, middle_x * along_y - middle_y * along_x)
        left[128 * j : 128 * (j + 1), :] = along.T.astype(jnp.bfloat16)
        left[BE + 128 * j : BE + 128 * (j + 1), :] = across.T.astype(jnp.bfloat16)

    row = lax.broadcasted_iota(jnp.int32, (128, 256), 0)
    lane = lax.broadcasted_iota(jnp.int32, (128, 256), 1)
    first = jnp.where(lane < 128, 24, 0)
    for j in range(TILES):
        inside = (row >= first) & (row < first + 24) & ((row & 7) == j)
        spreader[j] = jnp.where(inside, 1.0, 0.0).astype(jnp.bfloat16)

    m_ref[...] = jnp.full_like(m_ref, UNSEEN)
    s_ref[...] = jnp.zeros_like(s_ref)
    t_ref[...] = jnp.zeros_like(t_ref)

    def block_of(q):
        return pairs[0, cycle, 0, q]

    def look_up(q):
        index = names[pl.ds(pl.multiple_of(8 * q, 8), 8), :].astype(jnp.int32)
        low = index & 127
        high = index >> 7
        bits = [((high >> b) & 1) == 1 for b in range(7)]

        def found(r, b):
            if b < 0:
                part = table2[8 * r : 8 * r + 8, :]
                return jnp.take_along_axis(part, low, axis=1, mode="promise_in_bounds")
            return jnp.where(bits[b], found(r + (1 << b), b - 1), found(r, b - 1))

        both = found(0, 6)
        return jnp.where(high >= 128, pltpu.roll(both, 4, 0), both)

    def set_right(q):
        p = block_of(q)
        here = sub8 == q
        zero = jnp.zeros((8, 128), jnp.float32)
        one = jnp.where(here, 1.0, 0.0)
        for n in range(8):
            at = pl.ds(8 * p + n, 1)
            part = [
                jnp.where(here, jnp.broadcast_to(spots[i, at, :], (8, 128)), 0.0) for i in range(6)
            ]
            x, y = part[:3], part[3:]
            rows = []
            for c in (x, y):
                rows += [c[0], c[1], c[0], c[1], c[2], c[0]]
            rows += [one, one, one, zero]
            right[:, 128 * n : 128 * (n + 1)] = jnp.concatenate(rows, axis=0).astype(jnp.bfloat16)

    def set_column(q):
        half = jnp.concatenate(
            [halves[pl.ds(8 * j + q, 1), :] for j in range(TILES)]
            + [jnp.zeros((8 - TILES, 128), jnp.float32)],
            axis=0,
        )
        rows = list(pieces(look_up(q))) + list(pieces(half))
        full = jnp.concatenate(rows + [jnp.zeros((80, 128), jnp.float32)], axis=0)
        column[...] = full.T.astype(jnp.bfloat16)

    def multiply(n):
        return jnp.dot(
            left[...], right[:, 256 * n : 256 * (n + 1)], preferred_element_type=jnp.float32
        )

    def set_spread():
        for j in range(TILES):
            spread[128 * j : 128 * (j + 1), :] = jnp.dot(
                column[...], spreader[j], preferred_element_type=jnp.float32
            )

    def add_up(p, n, buf):
        m, s, t = [None, None], [None, None], [None, None]
        for g in range(BE // 8):
            up, down = slice(8 * g, 8 * g + 8), slice(BE + 8 * g, BE + 8 * g + 8)
            half = spread[up, 0:128]
            value = spread[up, 128:256]
            for h in range(2):
                at = slice(128 * h, 128 * (h + 1))
                d = squared_distance(buf[up, at], buf[down, at], half)
                w = jnp.exp2(OFFSET - d)
                m[h] = jnp.minimum(m[h], d) if g else d
                s[h] = s[h] + w if g else w
                t[h] = t[h] + w * value if g else w * value
        for h in range(2):
            here = pl.ds(8 * p + (2 * n + h), 1)
            m_ref[here, :] = jnp.minimum(m_ref[here, :], jnp.min(m[h], axis=0, keepdims=True))
            s_ref[here, :] = s_ref[here, :] + jnp.sum(s[h], axis=0, keepdims=True)
            t_ref[here, :] = t_ref[here, :] + jnp.sum(t[h], axis=0, keepdims=True)

    set_right(0)
    even[...] = multiply(0)
    set_column(0)
    set_spread()

    def slot(q, carry):
        p = block_of(q)
        later = jnp.minimum(q + 1, total - 1)
        one = multiply(1)
        add_up(p, 0, even)
        two = multiply(2)
        add_up(p, 1, one)
        three = multiply(3)
        add_up(p, 2, two)
        set_right(later)
        set_column(later)
        even[...] = multiply(0)
        add_up(p, 3, three)
        set_spread()
        return carry

    lax.fori_loop(0, total, slot, 0)

    def finish(*result):
        if cycle:
            result = combine(result, unpack(prior))
        for i, part in enumerate(result):
            out[64 * i : 64 * (i + 1), :] = part

    m = m_ref[...]
    seen = m < 0.5 * UNSEEN
    unsafe = jnp.max(jnp.where(seen & (m > SAFE), 1.0, 0.0)) > 0.0
    back = jnp.exp2(jnp.where(seen, m, OFFSET) - OFFSET)
    finish(jnp.where(seen, m, FAR), s_ref[...] * back, t_ref[...] * back)

    @pl.when(unsafe)
    def _():
        m_ref[...] = jnp.full_like(m_ref, FAR)
        s_ref[...] = jnp.zeros_like(s_ref)
        t_ref[...] = jnp.zeros_like(t_ref)

        def far_slot(q, carry):
            set_right(q)
            set_column(q)
            set_spread()
            for n in range(4):
                even[...] = multiply(n)
                for h in range(2):
                    at = slice(128 * h, 128 * (h + 1))

                    def terms(g):
                        up = pl.ds(pl.multiple_of(8 * g, 8), 8)
                        down = pl.ds(pl.multiple_of(BE + 8 * g, 8), 8)
                        d = squared_distance(even[up, at], even[down, at], spread[up, 0:128])
                        return d, spread[up, 128:256]

                    def lower(g, m):
                        return jnp.minimum(m, terms(g)[0])

                    least = jnp.full((8, 128), UNSEEN, jnp.float32)
                    least = lax.fori_loop(0, BE // 8, lower, least)
                    least = jnp.min(least, axis=0, keepdims=True)

                    def add(g, sums):
                        d, value = terms(g)
                        w = jnp.exp2(least - d)
                        return sums[0] + w, sums[1] + w * value

                    zero = jnp.zeros((8, 128), jnp.float32)
                    sums = lax.fori_loop(0, BE // 8, add, (zero, zero))
                    new = (least, *(jnp.sum(x, axis=0, keepdims=True) for x in sums))
                    here = pl.ds(8 * block_of(q) + (2 * n + h), 1)
                    old = (m_ref[here, :], s_ref[here, :], t_ref[here, :])
                    m_ref[here, :], s_ref[here, :], t_ref[here, :] = combine(old, new)
            return carry

        lax.fori_loop(0, total, far_slot, 0)
        finish(m_ref[...], s_ref[...], t_ref[...])


def join(cycle, block_pairs, live_slots, points, table, *sources):
    body = lambda *refs: join_kernel(cycle, *refs)
    bf16, f32 = jnp.bfloat16, jnp.float32
    pairs = 8.0 * BP * BE
    return pl.pallas_call(
        body,
        out_shape=jax.ShapeDtypeStruct((192, 128), f32),
        in_specs=[SMEM] * 2 + [VMEM] * (2 + len(sources)),
        out_specs=VMEM,
        scratch_shapes=[
            pltpu.VMEM((16 * SLOTS, 128), f32),
            pltpu.VMEM((8 * SLOTS, 128), f32),
            pltpu.VMEM((6, 64, 128), f32),
            pltpu.VMEM((1024, 128), f32),
            pltpu.VMEM((32, 128), f32),
            pltpu.VMEM((2 * BE, 128), bf16),
            pltpu.VMEM((128, BP), bf16),
            pltpu.VMEM((128, 128), bf16),
            pltpu.VMEM((TILES, 128, 256), bf16),
        ]
        + [pltpu.VMEM((BE, 256), f32)]
        + [pltpu.VMEM((2 * BE, 256), f32)]
        + [pltpu.VMEM((64, 128), f32)] * 3,
        compiler_params=pltpu.CompilerParams(vmem_limit_bytes=40 << 20),
        cost_estimate=pl.CostEstimate(
            flops=int(20 * pairs), bytes_accessed=1 << 20, transcendentals=int(pairs)
        ),
    )(block_pairs, live_slots, points, table, *sources)


def combine(one, other):
    least = jnp.minimum(one[0], other[0])
    share = jnp.exp2(least - one[0])
    other_share = jnp.exp2(least - other[0])
    return (
        least,
        one[1] * share + other[1] * other_share,
        one[2] * share + other[2] * other_share,
    )


def unpack(state):
    return state[0:64, :], state[64:128, :], state[128:192, :]


def steps(points, segments, edge_polygon, polygon_value, block_pairs, live_slots):
    mine = packed_cell(segments, edge_polygon)
    inner = lambda shard: swapped(shard, "pts", lambda c: c ^ 1)
    outer = lambda shard: swapped(shard, "pts", lambda c: ((c + 1) ^ 1) - 1)
    args = (block_pairs, live_slots, points, polygon_value.reshape(-1, 128))
    near1 = inner(mine)
    far1 = outer(mine)
    far2 = outer(near1)
    part = join(0, *args, mine)
    far1, part = lax.optimization_barrier((far1, part))
    near2 = inner(far1)
    part = join(1, *args, near1, far1, part)
    part = join(2, *args, near2, far2, part)
    state = unpack(part)
    for flip in (2, 3, 1):
        theirs = swapped(part, "poly", lambda q: q ^ flip)
        state = combine(state, unpack(theirs))
    state = combine(state, (FAR, 1.0, 0.0))
    return (state[0] * (1.0 / SCALE)).reshape(-1), (state[2] / state[1]).reshape(-1)


def solution(mesh):
    placed = (
        P(None, "pts"),
        P(None, ("pts", "poly")),
        P(("pts", "poly")),
        P(),
        P("pts", None, None, None),
        P("pts", None),
    )
    return jax.shard_map(
        steps, mesh=mesh, in_specs=placed, out_specs=(P("pts"), P("pts")), check_vma=False
    )
```

```python
import math

import jax
import jax.numpy as jnp
from jax import lax
from jax.experimental import pallas as pl
from jax.experimental.pallas import tpu as pltpu
from jax.sharding import PartitionSpec as P


BP = 1024
BE = 512
EB = 64
SLOTS = 8
CUTOFF = 9.0
SCALE = 256.0 / 9.0 / math.log(2.0)
ROOT = math.sqrt(SCALE)
FAR = CUTOFF * SCALE
OFFSET = 110.0
SAFE = 200.0
UNSEEN = 1.0e30

SMEM = pl.BlockSpec(memory_space=pltpu.SMEM)
VMEM = pl.BlockSpec(memory_space=pltpu.VMEM)


def swapped(shard, axis, partner):
    devices = lax.axis_size(axis)
    pairs = [(i, partner(i)) for i in range(devices) if 0 <= partner(i) < devices]
    return lax.ppermute(shard, axis, pairs)


def pack_kernel(corners, polygons, out):
    out[0:1024, :] = corners[...]
    out[1024:1280, :] = polygons[...].astype(jnp.float32)


def packed_cell(segments, edge_polygon):
    corners = segments.reshape(4, -1, 128).transpose(1, 0, 2).reshape(-1, 128)
    return pl.pallas_call(
        pack_kernel,
        out_shape=jax.ShapeDtypeStruct((1280, 128), jnp.float32),
        in_specs=[VMEM] * 2,
        out_specs=VMEM,
        compiler_params=pltpu.CompilerParams(vmem_limit_bytes=4 << 20),
        cost_estimate=pl.CostEstimate(flops=1 << 20, bytes_accessed=1 << 21, transcendentals=0),
        name="pack",
    )(corners, edge_polygon.reshape(-1, 128))


def pieces(x):
    first = x.astype(jnp.bfloat16).astype(jnp.float32)
    rest = x - first
    second = rest.astype(jnp.bfloat16).astype(jnp.float32)
    return first, second, rest - second


def affine_rows(x_factor, y_factor, constant):
    x, y, c = pieces(x_factor), pieces(y_factor), pieces(constant)
    zero = jnp.zeros_like(x_factor)
    rows = [x[0], x[0], x[1], x[1], x[0], x[2], y[0], y[0], y[1], y[1], y[0], y[2], c[0], c[1], c[2], zero]
    return jnp.concatenate(rows, axis=0)


def squared_distance(u, v, half):
    beyond = jnp.maximum(jnp.abs(u) - half, 0.0)
    return v * v + beyond * beyond


TILES = BE // 128


def join_kernel(cycle, pairs, live, points, table, *refs):
    if cycle == 0:
        (near, out), scratch = refs[:2], refs[2:]
    else:
        (near, far, prior, out), scratch = refs[:4], refs[4:]
    raw, names, spots, table2, halves, left, right, column, spreader = scratch[:9]
    spread, even, odd, m_ref, s_ref, t_ref = scratch[9:]
    sub8 = lax.broadcasted_iota(jnp.int32, (8, 128), 0)
    total = live[0, cycle]

    for s in range(SLOTS):
        name = pairs[0, cycle, 1, s]
        block = name & (EB - 1)
        corner_rows = pl.ds(pl.multiple_of(16 * block, 16), 16)
        name_rows = pl.ds(1024 + 4 * block, 4)
        corner, polygon = near[corner_rows, :], near[name_rows, :]
        if cycle:
            below_is_near = (lax.axis_index("pts") & 1) == 1
            take_near = (name < EB) == below_is_near
            corner = jnp.where(take_near, corner, far[corner_rows, :])
            polygon = jnp.where(take_near, polygon, far[name_rows, :])
        raw[16 * s : 16 * s + 16, :] = corner
        names[8 * s : 8 * s + 4, :] = polygon
        names[8 * s + 4 : 8 * s + 8, :] = polygon

    for r in range(128):
        one = jnp.broadcast_to(table[r : r + 1, :], (8, 128))
        other = jnp.broadcast_to(table[r + 128 : r + 129, :], (8, 128))
        table2[8 * r : 8 * r + 8, :] = jnp.where(sub8 < 4, one, other)

    for i in range(64):
        for c in range(2):
            spots[3 * c, i : i + 1, :] = points[c : c + 1, 128 * i : 128 * (i + 1)]
    centre_x = points[0:1, 0:1]
    for c, centre in ((0, centre_x), (1, 0.5)):
        for i, piece in enumerate(pieces(spots[3 * c] - centre)):
            spots[3 * c + i] = piece

    for j in range(TILES):
        start_x, start_y, end_x, end_y = (
            raw[pl.ds(4 * j + c, SLOTS, stride=16), :] for c in range(4)
        )
        delta_x = end_x - start_x
        delta_y = end_y - start_y
        middle_x = (start_x - centre_x) + 0.5 * delta_x
        middle_y = (start_y - 0.5) + 0.5 * delta_y
        squared = jnp.maximum(delta_x * delta_x + delta_y * delta_y, 1e-12)
        inverse = lax.rsqrt(squared) * ROOT
        along_x = delta_x * inverse
        along_y = delta_y * inverse
        halves[8 * j : 8 * j + 8, :] = 0.5 * squared * inverse
        along = affine_rows(along_x, along_y, -(middle_x * along_x + middle_y * along_y))
        across = affine_rows(-along_y, along_x, middle_x * along_y - middle_y * along_x)
        left[128 * j : 128 * (j + 1), :] = along.T.astype(jnp.bfloat16)
        left[BE + 128 * j : BE + 128 * (j + 1), :] = across.T.astype(jnp.bfloat16)

    row = lax.broadcasted_iota(jnp.int32, (128, 256), 0)
    lane = lax.broadcasted_iota(jnp.int32, (128, 256), 1)
    first = jnp.where(lane < 128, 24, 0)
    for j in range(TILES):
        inside = (row >= first) & (row < first + 24) & ((row & 7) == j)
        spreader[j] = jnp.where(inside, 1.0, 0.0).astype(jnp.bfloat16)

    m_ref[...] = jnp.full_like(m_ref, UNSEEN)
    s_ref[...] = jnp.zeros_like(s_ref)
    t_ref[...] = jnp.zeros_like(t_ref)

    def block_of(q):
        return pairs[0, cycle, 0, q]

    def look_up(q):
        index = names[pl.ds(pl.multiple_of(8 * q, 8), 8), :].astype(jnp.int32)
        low = index & 127
        high = index >> 7
        bits = [((high >> b) & 1) == 1 for b in range(7)]

        def found(r, b):
            if b < 0:
                part = table2[8 * r : 8 * r + 8, :]
                return jnp.take_along_axis(part, low, axis=1, mode="promise_in_bounds")
            return jnp.where(bits[b], found(r + (1 << b), b - 1), found(r, b - 1))

        both = found(0, 6)
        return jnp.where(high >= 128, pltpu.roll(both, 4, 0), both)

    def set_right(q):
        p = block_of(q)
        here = sub8 == q
        zero = jnp.zeros((8, 128), jnp.float32)
        one = jnp.where(here, 1.0, 0.0)
        for n in range(8):
            at = pl.ds(8 * p + n, 1)
            part = [
                jnp.where(here, jnp.broadcast_to(spots[i, at, :], (8, 128)), 0.0) for i in range(6)
            ]
            x, y = part[:3], part[3:]
            rows = []
            for c in (x, y):
                rows += [c[0], c[1], c[0], c[1], c[2], c[0]]
            rows += [one, one, one, zero]
            right[:, 128 * n : 128 * (n + 1)] = jnp.concatenate(rows, axis=0).astype(jnp.bfloat16)

    def set_column(q):
        half = jnp.concatenate(
            [halves[pl.ds(8 * j + q, 1), :] for j in range(TILES)]
            + [jnp.zeros((8 - TILES, 128), jnp.float32)],
            axis=0,
        )
        rows = list(pieces(look_up(q))) + list(pieces(half))
        full = jnp.concatenate(rows + [jnp.zeros((80, 128), jnp.float32)], axis=0)
        column[...] = full.T.astype(jnp.bfloat16)

    def multiply(n, buf):
        buf[...] = jnp.dot(
            left[...], right[:, 256 * n : 256 * (n + 1)], preferred_element_type=jnp.float32
        )

    def set_spread():
        for j in range(TILES):
            spread[128 * j : 128 * (j + 1), :] = jnp.dot(
                column[...], spreader[j], preferred_element_type=jnp.float32
            )

    def add_up(p, n, buf):
        m, s, t = [None, None], [None, None], [None, None]
        for g in range(BE // 8):
            up, down = slice(8 * g, 8 * g + 8), slice(BE + 8 * g, BE + 8 * g + 8)
            half = spread[up, 0:128]
            value = spread[up, 128:256]
            for h in range(2):
                at = slice(128 * h, 128 * (h + 1))
                d = squared_distance(buf[up, at], buf[down, at], half)
                w = jnp.exp2(OFFSET - d)
                m[h] = jnp.minimum(m[h], d) if g else d
                s[h] = s[h] + w if g else w
                t[h] = t[h] + w * value if g else w * value
        for h in range(2):
            here = pl.ds(8 * p + (2 * n + h), 1)
            m_ref[here, :] = jnp.minimum(m_ref[here, :], jnp.min(m[h], axis=0, keepdims=True))
            s_ref[here, :] = s_ref[here, :] + jnp.sum(s[h], axis=0, keepdims=True)
            t_ref[here, :] = t_ref[here, :] + jnp.sum(t[h], axis=0, keepdims=True)

    set_right(0)
    multiply(0, even)
    set_column(0)
    set_spread()

    def slot(q, carry):
        p = block_of(q)
        later = jnp.minimum(q + 1, total - 1)
        multiply(1, odd)
        add_up(p, 0, even)
        multiply(2, even)
        add_up(p, 1, odd)
        multiply(3, odd)
        add_up(p, 2, even)
        set_right(later)
        set_column(later)
        multiply(0, even)
        add_up(p, 3, odd)
        set_spread()
        return carry

    lax.fori_loop(0, total, slot, 0)

    def finish(*result):
        if cycle:
            result = combine(result, unpack(prior))
        for i, part in enumerate(result):
            out[64 * i : 64 * (i + 1), :] = part

    m = m_ref[...]
    seen = m < 0.5 * UNSEEN
    unsafe = jnp.max(jnp.where(seen & (m > SAFE), 1.0, 0.0)) > 0.0
    back = jnp.exp2(jnp.where(seen, m, OFFSET) - OFFSET)
    finish(jnp.where(seen, m, FAR), s_ref[...] * back, t_ref[...] * back)

    @pl.when(unsafe)
    def _():
        m_ref[...] = jnp.full_like(m_ref, FAR)
        s_ref[...] = jnp.zeros_like(s_ref)
        t_ref[...] = jnp.zeros_like(t_ref)

        def far_slot(q, carry):
            set_right(q)
            set_column(q)
            set_spread()
            for n in range(4):
                multiply(n, even)
                for h in range(2):
                    at = slice(128 * h, 128 * (h + 1))

                    def terms(g):
                        up = pl.ds(pl.multiple_of(8 * g, 8), 8)
                        down = pl.ds(pl.multiple_of(BE + 8 * g, 8), 8)
                        d = squared_distance(even[up, at], even[down, at], spread[up, 0:128])
                        return d, spread[up, 128:256]

                    def lower(g, m):
                        return jnp.minimum(m, terms(g)[0])

                    least = jnp.full((8, 128), UNSEEN, jnp.float32)
                    least = lax.fori_loop(0, BE // 8, lower, least)
                    least = jnp.min(least, axis=0, keepdims=True)

                    def add(g, sums):
                        d, value = terms(g)
                        w = jnp.exp2(least - d)
                        return sums[0] + w, sums[1] + w * value

                    zero = jnp.zeros((8, 128), jnp.float32)
                    sums = lax.fori_loop(0, BE // 8, add, (zero, zero))
                    new = (least, *(jnp.sum(x, axis=0, keepdims=True) for x in sums))
                    here = pl.ds(8 * block_of(q) + (2 * n + h), 1)
                    old = (m_ref[here, :], s_ref[here, :], t_ref[here, :])
                    m_ref[here, :], s_ref[here, :], t_ref[here, :] = combine(old, new)
            return carry

        lax.fori_loop(0, total, far_slot, 0)
        finish(m_ref[...], s_ref[...], t_ref[...])


def join(cycle, block_pairs, live_slots, points, table, *sources):
    body = lambda *refs: join_kernel(cycle, *refs)
    bf16, f32 = jnp.bfloat16, jnp.float32
    pairs = 8.0 * BP * BE
    return pl.pallas_call(
        body,
        out_shape=jax.ShapeDtypeStruct((192, 128), f32),
        in_specs=[SMEM] * 2 + [VMEM] * (2 + len(sources)),
        out_specs=VMEM,
        scratch_shapes=[
            pltpu.VMEM((16 * SLOTS, 128), f32),
            pltpu.VMEM((8 * SLOTS, 128), f32),
            pltpu.VMEM((6, 64, 128), f32),
            pltpu.VMEM((1024, 128), f32),
            pltpu.VMEM((32, 128), f32),
            pltpu.VMEM((2 * BE, 128), bf16),
            pltpu.VMEM((128, BP), bf16),
            pltpu.VMEM((128, 128), bf16),
            pltpu.VMEM((TILES, 128, 256), bf16),
        ]
        + [pltpu.VMEM((BE, 256), f32)]
        + [pltpu.VMEM((2 * BE, 256), f32)] * 2
        + [pltpu.VMEM((64, 128), f32)] * 3,
        compiler_params=pltpu.CompilerParams(vmem_limit_bytes=40 << 20),
        cost_estimate=pl.CostEstimate(
            flops=int(20 * pairs), bytes_accessed=1 << 20, transcendentals=int(pairs)
        ),
    )(block_pairs, live_slots, points, table, *sources)


def combine(one, other):
    least = jnp.minimum(one[0], other[0])
    share = jnp.exp2(least - one[0])
    other_share = jnp.exp2(least - other[0])
    return (
        least,
        one[1] * share + other[1] * other_share,
        one[2] * share + other[2] * other_share,
    )


def unpack(state):
    return state[0:64, :], state[64:128, :], state[128:192, :]


def steps(points, segments, edge_polygon, polygon_value, block_pairs, live_slots):
    mine = packed_cell(segments, edge_polygon)
    inner = lambda shard: swapped(shard, "pts", lambda c: c ^ 1)
    outer = lambda shard: swapped(shard, "pts", lambda c: ((c + 1) ^ 1) - 1)
    args = (block_pairs, live_slots, points, polygon_value.reshape(-1, 128))
    near1 = inner(mine)
    far1 = outer(mine)
    far2 = outer(near1)
    part = join(0, *args, mine)
    far1, part = lax.optimization_barrier((far1, part))
    near2 = inner(far1)
    part = join(1, *args, near1, far1, part)
    part = join(2, *args, near2, far2, part)
    state = unpack(part)
    for flip in (2, 3, 1):
        theirs = swapped(part, "poly", lambda q: q ^ flip)
        state = combine(state, unpack(theirs))
    state = combine(state, (FAR, 1.0, 0.0))
    return (state[0] * (1.0 / SCALE)).reshape(-1), (state[2] / state[1]).reshape(-1)


def solution(mesh):
    placed = (
        P(None, "pts"),
        P(None, ("pts", "poly")),
        P(("pts", "poly")),
        P(),
        P("pts", None, None, None),
        P("pts", None),
    )
    return jax.shard_map(
        steps, mesh=mesh, in_specs=placed, out_specs=(P("pts"), P("pts")), check_vma=False
    )
```

```python
import math

import jax
import jax.numpy as jnp
from jax import lax
from jax.experimental import pallas as pl
from jax.experimental.pallas import tpu as pltpu
from jax.sharding import PartitionSpec as P


BP = 1024
BE = 512
EB = 64
SLOTS = 8
CUTOFF = 9.0
SCALE = 256.0 / 9.0 / math.log(2.0)
ROOT = math.sqrt(SCALE)
FAR = CUTOFF * SCALE
OFFSET = 110.0
SAFE = 200.0
UNSEEN = 1.0e30

SMEM = pl.BlockSpec(memory_space=pltpu.SMEM)
VMEM = pl.BlockSpec(memory_space=pltpu.VMEM)


def swapped(shard, axis, partner):
    devices = lax.axis_size(axis)
    pairs = [(i, partner(i)) for i in range(devices) if 0 <= partner(i) < devices]
    return lax.ppermute(shard, axis, pairs)


def pack_kernel(corners, polygons, out, names, sems):
    first = pltpu.make_async_copy(corners, out.at[pl.ds(0, 1024), :], sems.at[0])
    second = pltpu.make_async_copy(polygons, names, sems.at[1])
    first.start()
    second.start()
    second.wait()
    out[1024:1280, :] = names[...].astype(jnp.float32)
    first.wait()


def packed_cell(segments, edge_polygon):
    corners = segments.reshape(4, -1, 128).transpose(1, 0, 2).reshape(-1, 128)
    return pl.pallas_call(
        pack_kernel,
        out_shape=jax.ShapeDtypeStruct((1280, 128), jnp.float32),
        in_specs=[pl.BlockSpec(memory_space=pltpu.HBM)] * 2,
        out_specs=VMEM,
        scratch_shapes=[pltpu.VMEM((256, 128), jnp.int32), pltpu.SemaphoreType.DMA((2,))],
        compiler_params=pltpu.CompilerParams(vmem_limit_bytes=4 << 20),
        cost_estimate=pl.CostEstimate(flops=1 << 20, bytes_accessed=1 << 21, transcendentals=0),
        name="pack",
    )(*(pltpu.with_memory_space_constraint(x, pltpu.HBM) for x in (corners, edge_polygon.reshape(-1, 128))))


def pieces(x):
    first = x.astype(jnp.bfloat16).astype(jnp.float32)
    rest = x - first
    second = rest.astype(jnp.bfloat16).astype(jnp.float32)
    return first, second, rest - second


def affine_rows(x_factor, y_factor, constant):
    x, y, c = pieces(x_factor), pieces(y_factor), pieces(constant)
    zero = jnp.zeros_like(x_factor)
    rows = [x[0], x[0], x[1], x[1], x[0], x[2], y[0], y[0], y[1], y[1], y[0], y[2], c[0], c[1], c[2], zero]
    return jnp.concatenate(rows, axis=0)


def squared_distance(u, v, half):
    beyond = jnp.maximum(jnp.abs(u) - half, 0.0)
    return v * v + beyond * beyond


TILES = BE // 128


def join_kernel(cycle, pairs, live, points, table, *refs):
    if cycle == 0:
        (near, out), scratch = refs[:2], refs[2:]
    else:
        (near, far, prior, out), scratch = refs[:4], refs[4:]
    raw, names, spots, table2, halves, left, right, column, spreader = scratch[:9]
    spread, even, odd, m_ref, s_ref, t_ref = scratch[9:]
    sub8 = lax.broadcasted_iota(jnp.int32, (8, 128), 0)
    total = live[0, cycle]

    for s in range(SLOTS):
        name = pairs[0, cycle, 1, s]
        block = name & (EB - 1)
        corner_rows = pl.ds(pl.multiple_of(16 * block, 16), 16)
        name_rows = pl.ds(1024 + 4 * block, 4)
        corner, polygon = near[corner_rows, :], near[name_rows, :]
        if cycle:
            below_is_near = (lax.axis_index("pts") & 1) == 1
            take_near = (name < EB) == below_is_near
            corner = jnp.where(take_near, corner, far[corner_rows, :])
            polygon = jnp.where(take_near, polygon, far[name_rows, :])
        raw[16 * s : 16 * s + 16, :] = corner
        names[8 * s : 8 * s + 4, :] = polygon
        names[8 * s + 4 : 8 * s + 8, :] = polygon

    for r in range(128):
        one = jnp.broadcast_to(table[r : r + 1, :], (8, 128))
        other = jnp.broadcast_to(table[r + 128 : r + 129, :], (8, 128))
        table2[8 * r : 8 * r + 8, :] = jnp.where(sub8 < 4, one, other)

    for i in range(64):
        for c in range(2):
            spots[3 * c, i : i + 1, :] = points[c : c + 1, 128 * i : 128 * (i + 1)]
    centre_x = points[0:1, 0:1]
    for c, centre in ((0, centre_x), (1, 0.5)):
        for i, piece in enumerate(pieces(spots[3 * c] - centre)):
            spots[3 * c + i] = piece

    for j in range(TILES):
        start_x, start_y, end_x, end_y = (
            raw[pl.ds(4 * j + c, SLOTS, stride=16), :] for c in range(4)
        )
        delta_x = end_x - start_x
        delta_y = end_y - start_y
        middle_x = (start_x - centre_x) + 0.5 * delta_x
        middle_y = (start_y - 0.5) + 0.5 * delta_y
        squared = jnp.maximum(delta_x * delta_x + delta_y * delta_y, 1e-12)
        inverse = lax.rsqrt(squared) * ROOT
        along_x = delta_x * inverse
        along_y = delta_y * inverse
        halves[8 * j : 8 * j + 8, :] = 0.5 * squared * inverse
        along = affine_rows(along_x, along_y, -(middle_x * along_x + middle_y * along_y))
        across = affine_rows(-along_y, along_x, middle_x * along_y - middle_y * along_x)
        left[128 * j : 128 * (j + 1), :] = along.T.astype(jnp.bfloat16)
        left[BE + 128 * j : BE + 128 * (j + 1), :] = across.T.astype(jnp.bfloat16)

    row = lax.broadcasted_iota(jnp.int32, (128, 256), 0)
    lane = lax.broadcasted_iota(jnp.int32, (128, 256), 1)
    first = jnp.where(lane < 128, 24, 0)
    for j in range(TILES):
        inside = (row >= first) & (row < first + 24) & ((row & 7) == j)
        spreader[j] = jnp.where(inside, 1.0, 0.0).astype(jnp.bfloat16)

    m_ref[...] = jnp.full_like(m_ref, UNSEEN)
    s_ref[...] = jnp.zeros_like(s_ref)
    t_ref[...] = jnp.zeros_like(t_ref)

    def block_of(q):
        return pairs[0, cycle, 0, q]

    def look_up(q):
        index = names[pl.ds(pl.multiple_of(8 * q, 8), 8), :].astype(jnp.int32)
        low = index & 127
        high = index >> 7
        bits = [((high >> b) & 1) == 1 for b in range(7)]

        def found(r, b):
            if b < 0:
                part = table2[8 * r : 8 * r + 8, :]
                return jnp.take_along_axis(part, low, axis=1, mode="promise_in_bounds")
            return jnp.where(bits[b], found(r + (1 << b), b - 1), found(r, b - 1))

        both = found(0, 6)
        return jnp.where(high >= 128, pltpu.roll(both, 4, 0), both)

    def set_right(q):
        p = block_of(q)
        here = sub8 == q
        zero = jnp.zeros((8, 128), jnp.float32)
        one = jnp.where(here, 1.0, 0.0)
        for n in range(8):
            at = pl.ds(8 * p + n, 1)
            part = [
                jnp.where(here, jnp.broadcast_to(spots[i, at, :], (8, 128)), 0.0) for i in range(6)
            ]
            x, y = part[:3], part[3:]
            rows = []
            for c in (x, y):
                rows += [c[0], c[1], c[0], c[1], c[2], c[0]]
            rows += [one, one, one, zero]
            right[:, 128 * n : 128 * (n + 1)] = jnp.concatenate(rows, axis=0).astype(jnp.bfloat16)

    def set_column(q):
        half = jnp.concatenate(
            [halves[pl.ds(8 * j + q, 1), :] for j in range(TILES)]
            + [jnp.zeros((8 - TILES, 128), jnp.float32)],
            axis=0,
        )
        rows = list(pieces(look_up(q))) + list(pieces(half))
        full = jnp.concatenate(rows + [jnp.zeros((80, 128), jnp.float32)], axis=0)
        column[...] = full.T.astype(jnp.bfloat16)

    def multiply(n, buf):
        buf[...] = jnp.dot(
            left[...], right[:, 256 * n : 256 * (n + 1)], preferred_element_type=jnp.float32
        )

    def set_spread():
        for j in range(TILES):
            spread[128 * j : 128 * (j + 1), :] = jnp.dot(
                column[...], spreader[j], preferred_element_type=jnp.float32
            )

    def add_up(p, n, buf):
        m, s, t = [None, None], [None, None], [None, None]
        for g in range(BE // 8):
            up, down = slice(8 * g, 8 * g + 8), slice(BE + 8 * g, BE + 8 * g + 8)
            half = spread[up, 0:128]
            value = spread[up, 128:256]
            for h in range(2):
                at = slice(128 * h, 128 * (h + 1))
                d = squared_distance(buf[up, at], buf[down, at], half)
                w = jnp.exp2(OFFSET - d)
                m[h] = jnp.minimum(m[h], d) if g else d
                s[h] = s[h] + w if g else w
                t[h] = t[h] + w * value if g else w * value
        for h in range(2):
            here = pl.ds(8 * p + (2 * n + h), 1)
            m_ref[here, :] = jnp.minimum(m_ref[here, :], jnp.min(m[h], axis=0, keepdims=True))
            s_ref[here, :] = s_ref[here, :] + jnp.sum(s[h], axis=0, keepdims=True)
            t_ref[here, :] = t_ref[here, :] + jnp.sum(t[h], axis=0, keepdims=True)

    set_right(0)
    multiply(0, even)
    set_column(0)
    set_spread()

    def slot(q, carry):
        p = block_of(q)
        later = jnp.minimum(q + 1, total - 1)
        multiply(1, odd)
        add_up(p, 0, even)
        multiply(2, even)
        add_up(p, 1, odd)
        multiply(3, odd)
        add_up(p, 2, even)
        set_right(later)
        set_column(later)
        multiply(0, even)
        add_up(p, 3, odd)
        set_spread()
        return carry

    lax.fori_loop(0, total, slot, 0)

    def finish(*result):
        if cycle:
            result = combine(result, unpack(prior))
        for i, part in enumerate(result):
            out[64 * i : 64 * (i + 1), :] = part

    m = m_ref[...]
    seen = m < 0.5 * UNSEEN
    unsafe = jnp.max(jnp.where(seen & (m > SAFE), 1.0, 0.0)) > 0.0
    back = jnp.exp2(jnp.where(seen, m, OFFSET) - OFFSET)
    finish(jnp.where(seen, m, FAR), s_ref[...] * back, t_ref[...] * back)

    @pl.when(unsafe)
    def _():
        m_ref[...] = jnp.full_like(m_ref, FAR)
        s_ref[...] = jnp.zeros_like(s_ref)
        t_ref[...] = jnp.zeros_like(t_ref)

        def far_slot(q, carry):
            set_right(q)
            set_column(q)
            set_spread()
            for n in range(4):
                multiply(n, even)
                for h in range(2):
                    at = slice(128 * h, 128 * (h + 1))

                    def terms(g):
                        up = pl.ds(pl.multiple_of(8 * g, 8), 8)
                        down = pl.ds(pl.multiple_of(BE + 8 * g, 8), 8)
                        d = squared_distance(even[up, at], even[down, at], spread[up, 0:128])
                        return d, spread[up, 128:256]

                    def lower(g, m):
                        return jnp.minimum(m, terms(g)[0])

                    least = jnp.full((8, 128), UNSEEN, jnp.float32)
                    least = lax.fori_loop(0, BE // 8, lower, least)
                    least = jnp.min(least, axis=0, keepdims=True)

                    def add(g, sums):
                        d, value = terms(g)
                        w = jnp.exp2(least - d)
                        return sums[0] + w, sums[1] + w * value

                    zero = jnp.zeros((8, 128), jnp.float32)
                    sums = lax.fori_loop(0, BE // 8, add, (zero, zero))
                    new = (least, *(jnp.sum(x, axis=0, keepdims=True) for x in sums))
                    here = pl.ds(8 * block_of(q) + (2 * n + h), 1)
                    old = (m_ref[here, :], s_ref[here, :], t_ref[here, :])
                    m_ref[here, :], s_ref[here, :], t_ref[here, :] = combine(old, new)
            return carry

        lax.fori_loop(0, total, far_slot, 0)
        finish(m_ref[...], s_ref[...], t_ref[...])


def join(cycle, block_pairs, live_slots, points, table, *sources):
    body = lambda *refs: join_kernel(cycle, *refs)
    bf16, f32 = jnp.bfloat16, jnp.float32
    pairs = 8.0 * BP * BE
    return pl.pallas_call(
        body,
        out_shape=jax.ShapeDtypeStruct((192, 128), f32),
        in_specs=[SMEM] * 2 + [VMEM] * (2 + len(sources)),
        out_specs=VMEM,
        scratch_shapes=[
            pltpu.VMEM((16 * SLOTS, 128), f32),
            pltpu.VMEM((8 * SLOTS, 128), f32),
            pltpu.VMEM((6, 64, 128), f32),
            pltpu.VMEM((1024, 128), f32),
            pltpu.VMEM((32, 128), f32),
            pltpu.VMEM((2 * BE, 128), bf16),
            pltpu.VMEM((128, BP), bf16),
            pltpu.VMEM((128, 128), bf16),
            pltpu.VMEM((TILES, 128, 256), bf16),
        ]
        + [pltpu.VMEM((BE, 256), f32)]
        + [pltpu.VMEM((2 * BE, 256), f32)] * 2
        + [pltpu.VMEM((64, 128), f32)] * 3,
        compiler_params=pltpu.CompilerParams(vmem_limit_bytes=40 << 20),
        cost_estimate=pl.CostEstimate(
            flops=int(20 * pairs), bytes_accessed=1 << 20, transcendentals=int(pairs)
        ),
    )(block_pairs, live_slots, points, table, *sources)


def combine(one, other):
    least = jnp.minimum(one[0], other[0])
    share = jnp.exp2(least - one[0])
    other_share = jnp.exp2(least - other[0])
    return (
        least,
        one[1] * share + other[1] * other_share,
        one[2] * share + other[2] * other_share,
    )


def unpack(state):
    return state[0:64, :], state[64:128, :], state[128:192, :]


def steps(points, segments, edge_polygon, polygon_value, block_pairs, live_slots):
    mine = packed_cell(segments, edge_polygon)
    inner = lambda shard: swapped(shard, "pts", lambda c: c ^ 1)
    outer = lambda shard: swapped(shard, "pts", lambda c: ((c + 1) ^ 1) - 1)
    args = (block_pairs, live_slots, points, polygon_value.reshape(-1, 128))
    near1 = inner(mine)
    far1 = outer(mine)
    far2 = outer(near1)
    part = join(0, *args, mine)
    far1, part = lax.optimization_barrier((far1, part))
    near2 = inner(far1)
    part = join(1, *args, near1, far1, part)
    part = join(2, *args, near2, far2, part)
    state = unpack(part)
    for flip in (2, 3, 1):
        theirs = swapped(part, "poly", lambda q: q ^ flip)
        state = combine(state, unpack(theirs))
    state = combine(state, (FAR, 1.0, 0.0))
    return (state[0] * (1.0 / SCALE)).reshape(-1), (state[2] / state[1]).reshape(-1)


def solution(mesh):
    placed = (
        P(None, "pts"),
        P(None, ("pts", "poly")),
        P(("pts", "poly")),
        P(),
        P("pts", None, None, None),
        P("pts", None),
    )
    return jax.shard_map(
        steps, mesh=mesh, in_specs=placed, out_specs=(P("pts"), P("pts")), check_vma=False
    )
```
